256 devices in a mesh: clip: 4 (over x, y), slab: 64 (over z, core).
Axes of the slice: x: 2, y: 2, z: 32, core: 2. Of those that a mesh axis runs over, the one named last changes fastest.
The devices are a block of a 4x8x32 slice.
Arguments:
- mask_field: float32 [8192, 2048], P(('clip', 'slab')), parts along dimension 0, may hold values from -1.8 to 2.9
- target_print: int32 [8192, 2048], P(('clip', 'slab')), parts along dimension 0, may hold values from 0 to 1
- source_points: int32 [64, 2], P('clip'), parts along dimension 0, may hold values from 0 to 60
- source_groups: int32 [64], P('clip'), parts along dimension 0, may hold values from 0 to 7
- group_logits: float32 [32], P('clip'), parts along dimension 0, may hold values from -1 to 1
- pupil_radius: int32 [4], P('clip'), parts along dimension 0, may hold values from 32 to 127
Outputs:
- loss_value: float32 [4], P('clip'), parts along dimension 0
- mask_grad: float32 [8192, 2048], P(('clip', 'slab')), parts along dimension 0
- group_grad: float32 [32], P('clip'), parts along dimension 0
The draws below stay inside these ranges and needn't reach their ends.
There are 4 independent parts, one for each index of `clip`. The reference program is written for one: setup_inputs(seed, part) draws one part's arguments, and reference() takes and returns one part's arrays. A program takes and returns all parts, laid end to end along the dimension named above; each array names one. Nothing has to cross between parts.
All inputs are finite; a program needn't handle non-finite values.
Results may differ from the reference program's by a relative error of at most 0.0003.
Values sent between devices are 32-bit elements; how exact they have to be, the bound alone decides.
No kernel may reach another device: no remote copies, remote signals or barrier semaphores. Data moves between devices by JAX's collectives and lax.ppermute only.
A program may use at most 128 MiB of HBM per device.

```python
import math
import jax
import jax.numpy as jnp
from jax import lax

N = 2048
K = 256
GRID = 61
NS = 16
NG = 8


def draw_mask_field(key, part):
    keys = jax.random.split(key, 5)
    rough = jax.random.uniform(keys[0], (N, N), jnp.float32)
    amplitude = jax.random.uniform(keys[1], (16,), jnp.float32, -1.0, 1.0)
    offset = 0.5
    wave_limit = 15 * K // 32
    first_wave = jax.random.randint(keys[2], (16,), -wave_limit, wave_limit + 1)
    second_wave = jax.random.randint(keys[3], (16,), -wave_limit, wave_limit + 1)
    phase_shift = jax.random.uniform(keys[4], (16,), jnp.float32, 0.0, 2.0 * math.pi)
    row_index = jnp.arange(N, dtype=jnp.int32)[:, None]
    col_index = jnp.arange(N, dtype=jnp.int32)[None, :]
    smooth = jnp.zeros((N, N), jnp.float32)
    for member in range(16):
        wrapped = jnp.mod(first_wave[member] * row_index + second_wave[member] * col_index, N)
        angles = 2.0 * math.pi * wrapped.astype(jnp.float32) / N + phase_shift[member]
        smooth = smooth + amplitude[member] * jnp.cos(angles)
    return offset + 0.12 * smooth + 0.3 * (2.0 * rough - 1.0)


def draw_target_print(key, part):
    row_index = jnp.arange(N, dtype=jnp.int32)[:, None]
    numbers = jax.random.randint(key, (N, N), 0, 1000)
    limit = 200 + 600 * row_index // N
    return (numbers < limit).astype(jnp.int32)


def with_ends(values, key, low, top_value):
    longest = values.shape.index(max(values.shape))
    spots = []
    for shift in (0, 1):
        where = [jax.random.randint(jax.random.fold_in(key, axis), (), 0, length) for axis, length in enumerate(values.shape)]
        where[longest] = (where[longest] + shift) % values.shape[longest]
        spots.append(tuple(where))
    return values.at[spots[0]].set(low).at[spots[1]].set(top_value)


def setup_inputs(seed: int = 0, part: int = 0) -> dict:
    key_of = jax.random.split(jax.random.key(seed), 7)
    part_keys = jax.random.split(jax.random.fold_in(key_of[6], part), 7)
    mask_field = draw_mask_field(jax.random.fold_in(jax.random.fold_in(key_of[6], part), 71), part)
    target_print = draw_target_print(jax.random.fold_in(jax.random.fold_in(key_of[6], part), 71), part)
    source_points = with_ends(jax.random.randint(part_keys[2], (NS, 2), 0, GRID), jax.random.fold_in(part_keys[2], 1), 0, GRID - 1).astype(jnp.int32)
    source_groups = with_ends(jax.random.randint(part_keys[3], (NS,), 0, NG), jax.random.fold_in(part_keys[3], 1), 0, NG - 1).astype(jnp.int32)
    group_logits = jnp.clip(jax.random.uniform(part_keys[4], (NG,), jnp.float32, -1.0, 1.0), -1.0, 1.0)
    pupil_radius = jax.random.randint(part_keys[5], (1,), K // 8, K // 2).astype(jnp.int32)
    return {"mask_field": mask_field, "target_print": target_print, "source_points": source_points, "source_groups": source_groups, "group_logits": group_logits, "pupil_radius": pupil_radius}


steepness = 8.0
threshold = 0.3
shift_scale = 45

def reference(mask_field, target_print, source_points, source_groups, group_logits, pupil_radius):
    half_band = K // 2
    frequency = jnp.arange(K, dtype=jnp.int32) - half_band
    band_index = jnp.mod(frequency, N).astype(jnp.int32)
    cutoff = pupil_radius[0].astype(jnp.int32)
    shifted = (source_points.astype(jnp.int32) - GRID // 2) * cutoff // shift_scale
    desired = target_print.astype(mask_field.dtype)

    def objective(field, logits):
        spectrum = jnp.fft.fft2(field)
        band = jnp.take(jnp.take(spectrum, band_index, axis=0), band_index, axis=1)
        weights = jnp.exp(logits[source_groups])
        total_weight = jnp.sum(weights)

        def add_source(running, source_item):
            offset, weight = source_item
            first_axis = frequency[:, None] + offset[0]
            second_axis = frequency[None, :] + offset[1]
            passed = first_axis * first_axis + second_axis * second_axis <= cutoff * cutoff
            clipped = jnp.where(passed, band, jnp.zeros_like(band))
            embedded = jnp.zeros((N, N), band.dtype).at[band_index[:, None], band_index[None, :]].set(clipped)
            image_field = jnp.fft.ifft2(embedded)
            bright = jnp.real(image_field) * jnp.real(image_field) + jnp.imag(image_field) * jnp.imag(image_field)
            return (running + weight * bright, None)
        running, unused = lax.scan(add_source, jnp.zeros((N, N), field.dtype), (shifted, weights))
        intensity = running / total_weight
        resist = jax.nn.sigmoid(steepness * (intensity - threshold))
        misfit = resist - desired
        return jnp.sum(misfit * misfit)
    total_sq, pullback = jax.vjp(objective, mask_field, group_logits)
    mask_grad, logit_grad = pullback(jnp.ones_like(total_sq))
    norming = 1.0 / (N * N)
    return ((total_sq * norming).reshape(1), mask_grad, logit_grad * norming)
```

```python
import functools

import numpy as np
import jax
import jax.numpy as jnp
from jax import lax
from jax.experimental import pallas as pl
from jax.experimental.pallas import tpu as pltpu
from jax.sharding import Mesh
from jax.sharding import PartitionSpec as P

K = 256
HALF = K // 2
GRID = 61
NG = 8
COARSE = 2 * K
PARCEL = 9 * 128
RING = "slab_0"
CORE = "slab_1"
SLAB = (RING, CORE)
CLIP_SLAB = ("clip", RING, CORE)

steepness = 8.0
threshold = 0.3
shift_scale = 45

f32 = jnp.float32
bf16 = jnp.bfloat16
NN = (((1,), (0,)), ((), ()))
NT = (((1,), (1,)), ((), ()))
TN = (((0,), (0,)), ((), ()))


def mm(a, b, dims=NN):
    return lax.dot_general(a, b, dims, preferred_element_type=f32)


def pieces(a):
    high = a.astype(bf16)
    return high, (a - high.astype(f32)).astype(bf16)


def mm3(a, b, dims=NN):
    return mm(a[0], b[0], dims) + mm(a[1], b[0], dims) + mm(a[0], b[1], dims)


def host_pieces(table):
    high = table.astype(np.float32).astype(jnp.bfloat16)
    low = (table - high.astype(np.float64)).astype(np.float32).astype(jnp.bfloat16)
    return np.asarray(high), np.asarray(low)


def turns(left, right, length):
    angle = 2.0 * np.pi * (np.outer(left, right) % length) / length
    return np.cos(angle), np.sin(angle)


def groups_of(e):
    return (e - 1) % 4, (3 - e) % 4


def lane_index(shape):
    return lax.broadcasted_iota(jnp.int32, shape, len(shape) - 1)


def row_index(shape):
    return lax.broadcasted_iota(jnp.int32, shape, 0)


def swapped(a, rows):
    lanes = a.shape[1]
    first = (lane_index(a.shape) // rows) % 2 == 0
    return jnp.where(first, pltpu.roll(a, lanes - rows, 1), -pltpu.roll(a, rows, 1))


def twiddle(cos_ref, sin_ref, m):
    owners = cos_ref.shape[0] - 8
    cos, sin = cos_ref[:owners], sin_ref[:owners]
    cos_m, sin_m = cos_ref[owners + m : owners + m + 1], sin_ref[owners + m : owners + m + 1]
    return cos * cos_m - sin * sin_m, sin * cos_m + cos * sin_m


def rows_kernel(mask_ref, high_ref, low_ref, out_ref):
    rows, length = mask_ref.shape
    quarter = length // 4
    m0, m1, m2, m3 = (mask_ref[:, q * quarter : (q + 1) * quarter] for q in range(4))
    even, odd = m0 + m2, m1 + m3
    stack = jnp.concatenate([even + odd, even - odd, m0 - m2, m1 - m3], 0)
    stack = pieces(stack)
    both = mm3((high_ref[...], low_ref[...]), stack, NT)
    cos, sin = both[:HALF], both[HALF:]
    c0, c2, ca, cb = (cos[:, i * rows : (i + 1) * rows] for i in range(4))
    s0, s2, sa, sb = (sin[:, i * rows : (i + 1) * rows] for i in range(4))
    owners = HALF // 2
    odd_row = row_index((owners, rows)) % 2 == 1
    lo, hi = slice(0, owners), slice(owners, HALF)
    ones = jnp.ones((owners, quarter), bf16)
    sums = (mm(ones, stack[0], NT) + mm(ones, stack[1], NT))[:, :rows]
    out_ref[:, :] = jnp.concatenate(
        [
            jnp.where(odd_row, c2[lo], ca[lo] - sb[lo]),
            jnp.where(odd_row, -s2[lo], -sa[lo] - cb[lo]),
            jnp.where(odd_row, c0[hi], ca[hi] + sb[hi]),
            jnp.where(odd_row, -s0[hi], cb[hi] - sa[hi]),
            sums,
            jnp.zeros((owners, 3 * rows), f32),
        ],
        1,
    )


def columns_kernel(in_ref, dft_high_ref, dft_low_ref, cos_ref, sin_ref, piece_ref, zero_ref):
    owners, lanes = in_ref.shape
    rows = lanes // 8
    a = in_ref[...]
    z = mm3((dft_high_ref[...], dft_low_ref[...]), pieces(jnp.concatenate([a, swapped(a, rows)], 0)))
    turned = swapped(z, rows)
    blocks = []
    for m in range(5):
        cos, sin = twiddle(cos_ref, sin_ref, m)
        cos = jnp.concatenate([cos, cos], 1)
        sin = jnp.concatenate([sin, sin], 1)
        blocks.append(z * cos + turned * sin)
    high, low = pieces(jnp.concatenate(blocks, 0))
    pick = (row_index((8, lanes)) == lane_index((8, lanes)) // rows).astype(f32).astype(bf16)
    sums = mm(pick, high, NT) + mm(pick, low, NT)
    copies = piece_ref.shape[0]
    lane = lane_index((copies, 128))
    tail = jnp.zeros((copies, 128), f32)
    for q in range(4):
        piece_ref[:, q * K : (q + 1) * K] = jnp.broadcast_to(sums[q : q + 1, :K], (copies, K))
        tail = jnp.where(lane == q, sums[q : q + 1, K : K + 1], tail)
    piece_ref[:, 4 * K :] = tail
    zero_ref[...] = sums[:, :K]


def image_kernel(
    shift_ref,
    share_ref,
    radius_ref,
    around_ref,
    zero_ref,
    local_p_ref,
    local_m_ref,
    local_pt_ref,
    local_mt_ref,
    field_high_ref,
    field_low_ref,
    spread_high_ref,
    spread_low_ref,
    target_ref,
    out_ref,
    plus_ref,
    minus_ref,
    lift_ref,
    field_ref,
    back_high_ref,
    back_low_ref,
    settled_ref,
    pull_p_ref,
    pull_m_ref,
    sums_ref,
):
    sources = shift_ref.shape[0]
    rows = target_ref.shape[0]
    half = 2 * rows
    norming = 1.0 / (target_ref.shape[1] * target_ref.shape[1])
    radius_sq = radius_ref[0] * radius_ref[0]
    wide = around_ref[...]
    body = jnp.concatenate([wide[:, : 2 * K], wide[:, 2 * K : 4 * K]], 0)
    spectrum = body.T
    tail = wide[:, 4 * K :].T
    zero = zero_ref[...].T
    lane = lane_index((1, HALF))
    ring = HALF // 4
    frequency = 4 * (lane % ring) + lane // ring + 1
    last = lane == HALF - 1
    frequency_p = jnp.where(last, 0, frequency)
    across = row_index((K, 1)) - HALF
    across_m = jnp.where(across == -HALF, HALF, across)
    last_col = lane_index((K, HALF)) == HALF - 1
    first_row = row_index((K, HALF)) == 0
    for part in range(2):
        block = spectrum[part * K : (part + 1) * K]
        plus = jnp.where(last_col, zero[:, 4 + part : 5 + part], block)
        edge = jnp.concatenate([tail[part : part + 1], tail[2 + part : 3 + part]], 1)
        minus = jnp.where(first_row, edge, block)
        for ref, value in ((plus_ref, plus), (minus_ref, minus)):
            high, low = pieces(value)
            ref[part * K : (part + 1) * K, :HALF] = high
            ref[part * K : (part + 1) * K, HALF:] = low

    def passes(s):
        s0 = shift_ref[s, 0]
        s1 = shift_ref[s, 1]
        a = across + s0
        b = frequency_p + s1
        plus = a * a <= radius_sq - b * b
        a = s0 - across_m
        b = s1 - frequency
        minus = a * a <= radius_sq - b * b
        return jnp.where(plus, 1.0, 0.0), jnp.where(minus, 1.0, 0.0)

    block = HALF // 4
    in_block = [lane_index((rows, HALF)) // block == i for i in range(4)]

    def place(choose):
        out = None
        for i in range(4):
            value, group = choose(i)
            value = pltpu.roll(value, (i - group) % 4 * block, 1) if i != group else value
            out = value if out is None else jnp.where(in_block[i], value, out)
        return out

    def lift(s, carry):
        parts = []
        for spec_ref, table_ref, passed in zip((plus_ref, minus_ref), (local_p_ref, local_m_ref), passes(s)):
            passed = passed.astype(bf16)
            passed = jnp.concatenate([passed, passed], 0)
            passed = jnp.concatenate([passed, passed], 1)
            out = mm(table_ref[...], spec_ref[...] * passed)
            out = (out[:half, :HALF] + out[half:, :HALF] + out[:half, HALF:]) * norming
            parts += [out[:rows], out[rows:]]
        at_rows = pl.ds(pl.multiple_of(s * rows, rows), rows)
        for e in range(4):
            groups = groups_of(e)
            high, low = pieces(place(lambda i: (parts[i], groups[i // 2])))
            lift_ref[at_rows, e * 2 * HALF : e * 2 * HALF + HALF] = high
            lift_ref[at_rows, e * 2 * HALF + HALF : (e + 1) * 2 * HALF] = low
        return carry

    lax.fori_loop(0, sources, lift, 0)
    field_tables = [
        (field_high_ref[e * HALF : (e + 1) * HALF], field_low_ref[e * HALF : (e + 1) * HALF]) for e in range(4)
    ]
    for e, (high, low) in enumerate(field_tables):
        lanes = slice(e * 2 * HALF, (e + 1) * 2 * HALF)
        packed = lift_ref[:, lanes]
        field_ref[:, lanes] = mm(packed, jnp.concatenate([high, high], 0)) + mm(packed[:, :HALF], low)

    def lane_blocks(at_rows):
        return [field_ref[at_rows, i * HALF : (i + 1) * HALF] for i in range(8)]

    def expose(s, total):
        at_rows = pl.ds(pl.multiple_of(s * rows, rows), rows)
        r0, i0, r1, i1, r2, i2, r3, i3 = lane_blocks(at_rows)
        real = [r0 + r2 + (r1 + r3), r0 - r2 - (i1 - i3), r0 + r2 - (r1 + r3), r0 - r2 + (i1 - i3)]
        imag = [i0 + i2 + (i1 + i3), i0 - i2 + (r1 - r3), i0 + i2 - (i1 + i3), i0 - i2 - (r1 - r3)]
        out = []
        for q in range(4):
            field_ref[at_rows, 2 * q * HALF : (2 * q + 1) * HALF] = real[q]
            field_ref[at_rows, (2 * q + 1) * HALF : (2 * q + 2) * HALF] = imag[q]
            out.append(total[q] + share_ref[s] * (real[q] * real[q] + imag[q] * imag[q]))
        return tuple(out)

    coarse = lax.fori_loop(0, sources, expose, (jnp.zeros((rows, HALF), f32),) * 4)
    spread = spread_high_ref[...], spread_low_ref[...]
    quarter = COARSE // 4
    spread = [tuple(t[at : at + n] for t in spread) for at, n in ((0, quarter), (quarter, quarter), (2 * quarter, 2 * quarter))]
    i0, i1, i2, i3 = coarse
    even, odd = i0 + i2, i1 + i3
    a, b = i0 - i2, i1 - i3
    e = mm3(pieces(even + odd), spread[0])
    f = mm3(pieces(even - odd), spread[1])
    rs = mm3(pieces(jnp.concatenate([jnp.concatenate([a, -b], 1), jnp.concatenate([b, a], 1)], 0)), spread[2])
    up, down = e + f, e - f
    r, t = rs[:rows], rs[rows:]
    fine = target_ref.shape[1] // 4
    slopes = []
    squares = jnp.zeros((rows, fine), f32)
    for q, intensity in enumerate((up + r, down + t, up - r, down - t)):
        resist = 1.0 / (1.0 + jnp.exp(-steepness * (intensity - threshold)))
        misfit = resist - target_ref[:, q * fine : (q + 1) * fine].astype(f32)
        slopes.append((2.0 * steepness) * misfit * resist * (1.0 - resist))
        squares = squares + misfit * misfit
    s0, s1, s2, s3 = slopes
    even, odd = s0 + s2, s1 + s3
    de = mm3(pieces(even + odd), spread[0], NT)
    df = mm3(pieces(even - odd), spread[1], NT)
    x = mm3(pieces(jnp.concatenate([s0 - s2, s1 - s3], 0)), spread[2], NT)
    da = x[:rows, :quarter] + x[rows:, quarter:]
    db = x[rows:, :quarter] - x[:rows, quarter:]
    up, down = de + df, de - df
    slope_c = [up + da, down + db, up - da, down - db]

    def lane_sum(a):
        a = jnp.sum(a, 0, keepdims=True)
        total = a[:, :128]
        for i in range(1, a.shape[1] // 128):
            total = total + a[:, i * 128 : (i + 1) * 128]
        return total

    sums_ref[...] = jnp.zeros(sums_ref.shape, f32)
    sums_ref[32:33, :] = lane_sum(squares)
    for ref in (pull_p_ref, pull_m_ref):
        ref[...] = jnp.zeros(ref.shape, f32)

    def push(s, carry):
        at_rows = pl.ds(pl.multiple_of(s * rows, rows), rows)
        blocks = lane_blocks(at_rows)
        bright = jnp.zeros((rows, HALF), f32)
        real, imag = [], []
        for q in range(4):
            re, im = blocks[2 * q], blocks[2 * q + 1]
            bright = bright + (re * re + im * im) * slope_c[q]
            factor = (2.0 * norming * share_ref[s]) * slope_c[q]
            real.append(factor * re)
            imag.append(factor * im)
        sums_ref[pl.ds(16 + s, 1), :] = jnp.sum(bright, 0, keepdims=True)
        er, ei, fr, fi = real[0] + real[2], imag[0] + imag[2], real[1] + real[3], imag[1] + imag[3]
        ar, ai, br, bi = real[0] - real[2], imag[0] - imag[2], real[1] - real[3], imag[1] - imag[3]
        turned = [er + fr, ei + fi, ar + bi, ai - br, er - fr, ei - fi, ar - bi, ai + br]
        for i, value in enumerate(turned):
            high, low = pieces(value)
            back_high_ref[at_rows, i * HALF : (i + 1) * HALF] = high
            back_low_ref[at_rows, i * HALF : (i + 1) * HALF] = low
        return carry

    lax.fori_loop(0, sources, push, 0)
    for e, (high, low) in enumerate(field_tables):
        lanes = slice(e * 2 * HALF, (e + 1) * 2 * HALF)
        both = mm(back_high_ref[:, lanes], jnp.concatenate([high, low], 0), NT)
        settled_ref[:, e * HALF : (e + 1) * HALF] = (
            both[:, :HALF] + both[:, HALF:] + mm(back_low_ref[:, lanes], high, NT)
        )

    def pull(s, carry):
        at_rows = pl.ds(pl.multiple_of(s * rows, rows), rows)
        settled = [settled_ref[at_rows, e * HALF : (e + 1) * HALF] for e in range(4)]
        arrays = [
            place(lambda i: (settled[(i + 1) % 4 if k < 2 else (3 - i) % 4], k)) for k in range(4)
        ]
        for pull_ref, table_ref, passed, at in zip(
            (pull_p_ref, pull_m_ref), (local_pt_ref, local_mt_ref), passes(s), (0, 2)
        ):
            high, low = pieces(jnp.concatenate(arrays[at : at + 2], 0))
            out = mm(table_ref[...], jnp.concatenate([high, low, high], 0))
            pull_ref[...] += out * jnp.concatenate([passed, passed], 0)
        return carry

    lax.fori_loop(0, sources, pull, 0)
    plus = pull_p_ref[...]
    minus = pull_m_ref[...]
    owners = HALF // 2
    sums = jnp.sum(sums_ref[...].T, 0, keepdims=True)
    lane = lane_index((owners, 128))
    tail = jnp.where(lane >= 16, sums, 0.0)
    for i in range(8):
        tail = jnp.where(lane == 8 + i, plus[i * owners : (i + 1) * owners, HALF - 1 :], tail)
    edge = jnp.concatenate([minus[:1], minus[K : K + 1], jnp.zeros((6, HALF), f32)], 0).T
    for j in range(2):
        for part in range(2):
            tail = jnp.where(lane == 2 * j + part, edge[j * owners : (j + 1) * owners, part : part + 1], tail)
    out_ref[:, 4 * K :] = tail
    total = jnp.where(lane_index(plus.shape) == HALF - 1, 0.0, plus)
    total = total + jnp.where(row_index(plus.shape) % K == 0, 0.0, minus)
    total = total.T
    out_ref[:, : 2 * K] = total[:owners]
    out_ref[:, 2 * K : 4 * K] = total[owners:]


def owner_kernel(in_ref, high_ref, low_ref, cos_ref, sin_ref, zero_cos_ref, zero_sin_ref, out_ref, sums_ref):
    total = jnp.sum(in_ref[...], 0, keepdims=True)
    tail = total[:, 4 * K :]
    sums_ref[...] = jnp.broadcast_to(tail, sums_ref.shape)
    owners = HALF // 2
    rows = cos_ref.shape[1] // 4
    quantities = [total[:, q * K : (q + 1) * K] for q in range(4)]
    columns = jnp.concatenate(quantities + [jnp.zeros((4, K), f32)], 0).T
    lane = lane_index((owners, 4 * rows))
    where = lane // rows
    z = jnp.zeros((owners, 4 * rows), f32)
    for m in range(5):
        cos, sin = twiddle(cos_ref, sin_ref, m)
        if m < 4:
            part = columns[m * owners : (m + 1) * owners]
            cols = [part[:, q : q + 1] for q in range(4)]
        else:
            top = row_index((owners, 1)) == 0
            cols = [jnp.where(top, tail[:, q : q + 1], 0.0) for q in range(4)]
        straight = jnp.where(where == 0, cols[0], jnp.where(where == 1, cols[1], jnp.where(where == 2, cols[2], cols[3])))
        crossed = jnp.where(where == 0, -cols[1], jnp.where(where == 1, cols[0], jnp.where(where == 2, -cols[3], cols[2])))
        z = z + straight * cos + crossed * sin
    out = mm3((high_ref[...], low_ref[...]), pieces(jnp.concatenate([z, -swapped(z, rows)], 0)))
    const = jnp.zeros((owners, 4 * rows), f32)
    real = jnp.zeros((owners, 4 * rows), f32)
    imag = jnp.zeros((owners, 4 * rows), f32)
    for i in range(4):
        real = jnp.where(where == i, tail[:, 8 + i : 9 + i], real)
        imag = jnp.where(where == i, tail[:, 12 + i : 13 + i], imag)
    const = real * zero_cos_ref[...] - imag * zero_sin_ref[...]
    const = const + pltpu.roll(const, 2 * rows, 1)
    const = const + pltpu.roll(const, rows, 1)
    out_ref[:, : 4 * rows] = out
    out_ref[:, 4 * rows :] = const


def grad_kernel(in_ref, high_ref, low_ref, out_ref):
    rows, length = out_ref.shape
    quarter = length // 4
    owners = in_ref.shape[0]
    a = in_ref[...]
    odd_row = row_index((owners, rows)) % 2 == 1
    none = jnp.zeros((owners, rows), f32)
    real0, imag0, real1, imag1 = (a[:, i * rows : (i + 1) * rows] for i in range(4))
    top = jnp.concatenate(
        [none, jnp.where(odd_row, real0, 0.0), jnp.where(odd_row, 0.0, real0), jnp.where(odd_row, 0.0, -imag0)], 1
    )
    top_sin = jnp.concatenate(
        [none, jnp.where(odd_row, -imag0, 0.0), jnp.where(odd_row, 0.0, -imag0), jnp.where(odd_row, 0.0, -real0)], 1
    )
    low = jnp.concatenate(
        [jnp.where(odd_row, real1, 0.0), none, jnp.where(odd_row, 0.0, real1), jnp.where(odd_row, 0.0, imag1)], 1
    )
    low_sin = jnp.concatenate(
        [jnp.where(odd_row, -imag1, 0.0), none, jnp.where(odd_row, 0.0, -imag1), jnp.where(odd_row, 0.0, real1)], 1
    )
    stack = jnp.concatenate([top, low, top_sin, low_sin], 0).T
    both = mm3(pieces(stack), (high_ref[...], low_ref[...]))
    const = jnp.sum(a[:, 4 * rows :].T, 1, keepdims=True)[:rows]
    e = both[:rows] + const
    f = both[rows : 2 * rows]
    g = both[2 * rows : 3 * rows]
    h = both[3 * rows :]
    up, down = e + f, e - f
    out_ref[:, :quarter] = up + g
    out_ref[:, quarter : 2 * quarter] = down + h
    out_ref[:, 2 * quarter : 3 * quarter] = up - g
    out_ref[:, 3 * quarter :] = down - h


def tables(rows, length, ring):
    owners = HALF // 2
    z = np.arange(ring)
    by_owner = np.stack([4 * z + c + 1 for c in range(2)], 1).reshape(-1)
    slots = np.concatenate([by_owner, by_owner + 2])
    cos, sin = turns(slots, np.arange(length // 4), length)
    row_table = np.concatenate([cos, sin], 0)
    cos, sin = turns(np.arange(owners), np.arange(owners), owners)
    dft = np.concatenate([cos, sin], 1)
    across = np.concatenate([np.arange(owners), owners * np.arange(8) - HALF])
    cos, sin = turns(across, np.arange(rows), length)
    turning = np.tile(cos, (1, 4)).astype(np.float32), np.tile(sin, (1, 4)).astype(np.float32)
    samples = (length // COARSE) * np.arange(COARSE)
    lanes = np.concatenate([4 * z + g + 1 for g in range(4)])
    first = np.concatenate([lanes[:-1], [0]])
    cos_p, sin_p = turns(first, samples[: COARSE // 4], length)
    cos_m, sin_m = turns(lanes, samples[: COARSE // 4], length)
    field = []
    for e in range(4):
        p, m = (slice(g * ring, (g + 1) * ring) for g in groups_of(e))
        real = np.concatenate([cos_p[p], -sin_p[p], cos_m[m], -sin_m[m]], 0)
        imag = np.concatenate([sin_p[p], cos_p[p], -sin_m[m], -cos_m[m]], 0)
        field.append(np.concatenate([real, imag], 1))
    field = np.concatenate(field, 0)
    tones = np.arange(1, COARSE // 2 + 1)
    share = np.where(tones == COARSE // 2, 1.0, 2.0)
    pixels = np.arange(length)
    kernel = (1.0 + np.cos(2.0 * np.pi * (np.outer(pixels, tones) % length) / length) @ share) / COARSE
    near, fine = samples[: COARSE // 4, None], pixels[None, : length // 4]
    h0, h1, h2, h3 = (kernel[(fine + p * (length // 4) - near) % length] for p in range(4))
    spread = np.concatenate([(h0 + h1 + h2 + h3) / 4, (h0 - h1 + h2 - h3) / 4, (h0 - h2) / 2, (h1 - h3) / 2], 0)
    return host_pieces(row_table), host_pieces(dft), turning, host_pieces(field), host_pieces(spread)


def call(kernel, out_shape, scratch=(), n_scalar=0, n_in=0, interpret=False, flops=0):
    vmem = pl.BlockSpec(memory_space=pltpu.VMEM)
    smem = pl.BlockSpec(memory_space=pltpu.SMEM)
    multi = isinstance(out_shape, (tuple, list))
    return pl.pallas_call(
        kernel,
        out_shape=out_shape,
        in_specs=[smem] * n_scalar + [vmem] * n_in,
        out_specs=[vmem] * len(out_shape) if multi else vmem,
        scratch_shapes=list(scratch),
        compiler_params=pltpu.CompilerParams(vmem_limit_bytes=56 * 1024 * 1024),
        interpret=interpret,
    )


INTERPRET = False


def on_device(mask_field, target_print, source_points, source_groups, group_logits, pupil_radius):
    rows, length = mask_field.shape
    ring = lax.axis_size(RING)
    pair = lax.axis_size(CORE)
    owners = ring * pair
    sources = source_points.shape[0]
    row_table, dft, turning, field, spread = tables(rows, length, ring)
    device = lax.axis_index(SLAB)
    norming = 1.0 / (length * length)
    cutoff = pupil_radius[0]
    shifted = (source_points - GRID // 2) * cutoff // shift_scale
    shape = functools.partial(jax.ShapeDtypeStruct, dtype=f32)
    run = functools.partial(call, interpret=INTERPRET)

    def swap_all(parcels, axes):
        return lax.all_to_all(parcels, axes, split_axis=0, concat_axis=0, tiled=True)

    parcels = run(rows_kernel, shape((owners, 8 * rows)), n_in=3)(mask_field, *row_table)
    arrived = swap_all(parcels, SLAB)
    piece, zero = run(columns_kernel, (shape((ring, PARCEL)), shape((8, K))), n_in=5)(arrived, *dft, *turning)
    around = swap_all(piece, RING)
    around = lax.all_gather(around, CORE).reshape(owners, PARCEL)

    onehot = (source_groups[:, None] == jnp.arange(NG, dtype=jnp.int32)[None, :]).astype(f32)
    weights = jnp.exp(jnp.sum(onehot * group_logits[None, :], 1))
    total_weight = jnp.sum(weights)
    weight_share = weights / total_weight
    across = jnp.arange(K, dtype=jnp.int32) - HALF
    across_m = jnp.where(across == -HALF, HALF, across)
    here = device * rows + jnp.arange(rows, dtype=jnp.int32)

    def local(freq):
        angle = jnp.mod(here[:, None] * freq[None, :], length).astype(f32) * (2.0 * np.pi / length)
        c, s = jnp.cos(angle), jnp.sin(angle)
        table = jnp.concatenate([jnp.concatenate([c, -s], 1), jnp.concatenate([s, c], 1)], 0)
        rounded = lax.reduce_precision(table, 8, 7)
        high, low = rounded.astype(bf16), (table - rounded).astype(bf16)
        return jnp.concatenate([high, low], 0), jnp.concatenate([high.T, high.T, low.T], 1)

    local_p, local_pt = local(across)
    local_m, local_mt = local(across_m)
    vmem = pltpu.VMEM
    out = run(
        image_kernel,
        shape((owners, PARCEL)),
        n_scalar=3,
        n_in=11,
        scratch=[
            vmem((2 * K, 2 * HALF), bf16),
            vmem((2 * K, 2 * HALF), bf16),
            vmem((sources * rows, 8 * HALF), bf16),
            vmem((sources * rows, 2 * COARSE), f32),
            vmem((sources * rows, 2 * COARSE), bf16),
            vmem((sources * rows, 2 * COARSE), bf16),
            vmem((sources * rows, 4 * HALF), f32),
            vmem((2 * K, HALF), f32),
            vmem((2 * K, HALF), f32),
            vmem((128, 128), f32),
        ],
    )(
        shifted,
        weight_share,
        pupil_radius,
        around,
        zero,
        local_p,
        local_m,
        local_pt,
        local_mt,
        *field,
        *spread,
        target_print,
    )
    parcels = out.reshape(pair, ring, PARCEL)
    mine = swap_all(parcels, CORE).sum(0)
    mine = swap_all(mine, RING)
    place = lax.axis_index(CORE) * ring + lax.axis_index(RING)
    own_across = place - HALF + owners * jnp.arange(K // owners, dtype=jnp.int32)
    pixels = jnp.arange(length, dtype=jnp.int32).reshape(owners, 1, rows)
    angle = jnp.mod(own_across[None, :, None] * pixels, length).astype(f32) * (2.0 * np.pi / length)
    zero_cos = jnp.cos(angle).reshape(owners, -1)
    zero_sin = jnp.sin(angle).reshape(owners, -1)
    parcels, sums = run(owner_kernel, (shape((owners, 8 * rows)), shape((8, 128))), n_in=7)(
        mine, *dft, *turning, zero_cos, zero_sin
    )
    arrived = swap_all(parcels, SLAB)
    mask_grad = run(grad_kernel, shape((rows, length)), n_in=3)(arrived, *row_table)
    per_source = sums[0, 16 : 16 + sources]
    squares = sums[0, 32]
    loss_value = (squares * norming).reshape(1)
    against = jnp.sum(weight_share * per_source)
    source_pull = weights * (per_source - against) / total_weight
    group_grad = jnp.sum(onehot * source_pull[:, None], 0) * norming
    return (loss_value, mask_grad, group_grad)


def solution(mesh):
    cores = 2
    ring = mesh.shape["slab"] // cores
    split = Mesh(mesh.devices.reshape(mesh.shape["clip"], ring, cores), CLIP_SLAB)
    return jax.shard_map(
        on_device,
        mesh=split,
        in_specs=(
            P(CLIP_SLAB, None),
            P(CLIP_SLAB, None),
            P("clip", None),
            P("clip"),
            P("clip"),
            P("clip"),
        ),
        out_specs=(P("clip"), P(CLIP_SLAB, None), P("clip")),
        check_vma=False,
    )
```

```python
import functools

import numpy as np
import jax
import jax.numpy as jnp
from jax import lax
from jax.experimental import pallas as pl
from jax.experimental.pallas import tpu as pltpu
from jax.sharding import Mesh
from jax.sharding import PartitionSpec as P

K = 256
HALF = K // 2
GRID = 61
NG = 8
COARSE = 2 * K
PARCEL = 9 * 128
RING = "slab_0"
CORE = "slab_1"
SLAB = (RING, CORE)
CLIP_SLAB = ("clip", RING, CORE)

steepness = 8.0
threshold = 0.3
shift_scale = 45

f32 = jnp.float32
bf16 = jnp.bfloat16
NN = (((1,), (0,)), ((), ()))
NT = (((1,), (1,)), ((), ()))
TN = (((0,), (0,)), ((), ()))


def mm(a, b, dims=NN):
    return lax.dot_general(a, b, dims, preferred_element_type=f32)


def pieces(a):
    high = a.astype(bf16)
    return high, (a - high.astype(f32)).astype(bf16)


def mm3(a, b, dims=NN):
    return mm(a[0], b[0], dims) + mm(a[1], b[0], dims) + mm(a[0], b[1], dims)


def host_pieces(table):
    high = table.astype(np.float32).astype(jnp.bfloat16)
    low = (table - high.astype(np.float64)).astype(np.float32).astype(jnp.bfloat16)
    return np.asarray(high), np.asarray(low)


def turns(left, right, length):
    angle = 2.0 * np.pi * (np.outer(left, right) % length) / length
    return np.cos(angle), np.sin(angle)


def groups_of(e):
    return (e - 1) % 4, (3 - e) % 4


def lane_index(shape):
    return lax.broadcasted_iota(jnp.int32, shape, len(shape) - 1)


def row_index(shape):
    return lax.broadcasted_iota(jnp.int32, shape, 0)


def swapped(a, rows):
    lanes = a.shape[1]
    first = (lane_index(a.shape) // rows) % 2 == 0
    return jnp.where(first, pltpu.roll(a, lanes - rows, 1), -pltpu.roll(a, rows, 1))


def twiddle(cos_ref, sin_ref, m):
    owners = cos_ref.shape[0] - 8
    cos, sin = cos_ref[:owners], sin_ref[:owners]
    cos_m, sin_m = cos_ref[owners + m : owners + m + 1], sin_ref[owners + m : owners + m + 1]
    return cos * cos_m - sin * sin_m, sin * cos_m + cos * sin_m


def rows_kernel(mask_ref, high_ref, low_ref, out_ref, sums_ref):
    rows, length = mask_ref.shape
    quarter = length // 4
    m0, m1, m2, m3 = (mask_ref[:, q * quarter : (q + 1) * quarter] for q in range(4))
    even, odd = m0 + m2, m1 + m3
    stack = jnp.concatenate([even + odd, even - odd, m0 - m2, m1 - m3], 0)
    stack = pieces(stack)
    both = mm3((high_ref[...], low_ref[...]), stack, NT)
    cos, sin = both[:HALF], both[HALF:]
    c0, c2, ca, cb = (cos[:, i * rows : (i + 1) * rows] for i in range(4))
    s0, s2, sa, sb = (sin[:, i * rows : (i + 1) * rows] for i in range(4))
    owners = HALF // 2
    odd_row = row_index((owners, rows)) % 2 == 1
    lo, hi = slice(0, owners), slice(owners, HALF)
    ones = jnp.ones((8, quarter), bf16)
    sums_ref[...] = (mm(ones, stack[0], NT) + mm(ones, stack[1], NT))[:1]
    parcels = jnp.concatenate(
        [
            jnp.where(odd_row, c2[lo], ca[lo] - sb[lo]),
            jnp.where(odd_row, -s2[lo], -sa[lo] - cb[lo]),
            jnp.where(odd_row, c0[hi], ca[hi] + sb[hi]),
            jnp.where(odd_row, -s0[hi], cb[hi] - sa[hi]),
        ],
        1,
    )
    out_ref[...] = parcels.reshape(out_ref.shape)


def columns_kernel(in_ref, own_sums_ref, dft_high_ref, dft_low_ref, cos_ref, sin_ref, piece_ref):
    owners, _, lanes = in_ref.shape
    rows = lanes // 4
    a = in_ref[...].reshape(owners, lanes)
    z = mm3((dft_high_ref[...], dft_low_ref[...]), pieces(jnp.concatenate([a, swapped(a, rows)], 0)))
    turned = swapped(z, rows)
    blocks = []
    for m in range(5):
        cos, sin = twiddle(cos_ref, sin_ref, m)
        blocks.append(z * cos + turned * sin)
    high, low = pieces(jnp.concatenate(blocks, 0))
    pick = (row_index((8, lanes)) == lane_index((8, lanes)) // rows).astype(f32).astype(bf16)
    sums = mm(pick, high, NT) + mm(pick, low, NT)
    copies = piece_ref.shape[0]
    lane = lane_index((1, 128))
    tail = jnp.where(lane // rows == 1, pltpu.roll(own_sums_ref[...], rows, 1), 0.0)
    for q in range(4):
        tail = jnp.where(lane == q, sums[q : q + 1, K : K + 1], tail)
    row = jnp.concatenate([sums[q : q + 1, :K] for q in range(4)] + [tail], 1)
    piece_ref[...] = jnp.broadcast_to(row.reshape(1, 1, PARCEL), (copies, 1, PARCEL))


def image_kernel(
    shift_ref,
    share_ref,
    radius_ref,
    core_ref,
    mine_ref,
    theirs_ref,
    turn_high_ref,
    turn_low_ref,
    cos_ref,
    sin_ref,
    local_p_ref,
    local_m_ref,
    local_pt_ref,
    local_mt_ref,
    field_high_ref,
    field_low_ref,
    spread_high_ref,
    spread_low_ref,
    target_ref,
    out_mine_ref,
    out_theirs_ref,
    plus_ref,
    minus_ref,
    lift_ref,
    field_ref,
    back_high_ref,
    back_low_ref,
    settled_ref,
    pull_p_ref,
    pull_m_ref,
    sums_ref,
):
    sources = shift_ref.shape[0]
    rows = target_ref.shape[0]
    half = 2 * rows
    norming = 1.0 / (target_ref.shape[1] * target_ref.shape[1])
    radius_sq = radius_ref[0] * radius_ref[0]
    first_core = core_ref[0] == 0
    ring = mine_ref.shape[0]
    mine = mine_ref[...].reshape(ring, PARCEL)
    theirs = theirs_ref[...].reshape(ring, PARCEL)
    wide = jnp.concatenate([jnp.where(first_core, mine, theirs), jnp.where(first_core, theirs, mine)], 0)
    body = jnp.concatenate([wide[:, : 2 * K], wide[:, 2 * K : 4 * K]], 0)
    spectrum = body.T
    tail = wide[:, 4 * K :].T
    turn = turn_high_ref[...], turn_low_ref[...]
    owners = 2 * ring
    z = mm3(turn, pieces(wide[:, 4 * K + rows : 4 * K + 2 * rows]), TN)
    z_real, z_imag = z[:owners], -z[owners:]
    turns_of = [tuple(t[:, :rows] for t in twiddle(cos_ref, sin_ref, m)) for m in range(4)]
    zero = [
        jnp.concatenate([jnp.sum(z_real * c + z_imag * n, 1, keepdims=True) for c, n in turns_of], 0),
        jnp.concatenate([jnp.sum(z_imag * c - z_real * n, 1, keepdims=True) for c, n in turns_of], 0),
    ]
    lane = lane_index((1, HALF))
    frequency = 4 * (lane % ring) + lane // ring + 1
    last = lane == HALF - 1
    frequency_p = jnp.where(last, 0, frequency)
    across = row_index((K, 1)) - HALF
    across_m = jnp.where(across == -HALF, HALF, across)
    last_col = lane_index((K, HALF)) == HALF - 1
    first_row = row_index((K, HALF)) == 0
    for part in range(2):
        block = spectrum[part * K : (part + 1) * K]
        plus = jnp.where(last_col, zero[part], block)
        edge = jnp.concatenate([tail[part : part + 1], tail[2 + part : 3 + part]], 1)
        minus = jnp.where(first_row, edge, block)
        for ref, value in ((plus_ref, plus), (minus_ref, minus)):
            high, low = pieces(value)
            ref[part * K : (part + 1) * K, :HALF] = high
            ref[part * K : (part + 1) * K, HALF:] = low

    def passes(s):
        s0 = shift_ref[s, 0]
        s1 = shift_ref[s, 1]
        a = across + s0
        b = frequency_p + s1
        plus = a * a <= radius_sq - b * b
        a = s0 - across_m
        b = s1 - frequency
        minus = a * a <= radius_sq - b * b
        return jnp.where(plus, 1.0, 0.0), jnp.where(minus, 1.0, 0.0)

    block = HALF // 4
    in_block = [lane_index((rows, HALF)) // block == i for i in range(4)]

    def place(choose):
        out = None
        for i in range(4):
            value, group = choose(i)
            value = pltpu.roll(value, (i - group) % 4 * block, 1) if i != group else value
            out = value if out is None else jnp.where(in_block[i], value, out)
        return out

    def lift(s, carry):
        parts = []
        for spec_ref, table_ref, passed in zip((plus_ref, minus_ref), (local_p_ref, local_m_ref), passes(s)):
            passed = passed.astype(bf16)
            passed = jnp.concatenate([passed, passed], 0)
            passed = jnp.concatenate([passed, passed], 1)
            out = mm(table_ref[...], spec_ref[...] * passed)
            out = (out[:half, :HALF] + out[half:, :HALF] + out[:half, HALF:]) * norming
            parts += [out[:rows], out[rows:]]
        at_rows = pl.ds(pl.multiple_of(s * rows, rows), rows)
        for e in range(4):
            groups = groups_of(e)
            high, low = pieces(place(lambda i: (parts[i], groups[i // 2])))
            lift_ref[at_rows, e * 2 * HALF : e * 2 * HALF + HALF] = high
            lift_ref[at_rows, e * 2 * HALF + HALF : (e + 1) * 2 * HALF] = low
        return carry

    lax.fori_loop(0, sources, lift, 0)
    field_tables = [
        (field_high_ref[e * HALF : (e + 1) * HALF], field_low_ref[e * HALF : (e + 1) * HALF]) for e in range(4)
    ]
    for e, (high, low) in enumerate(field_tables):
        lanes = slice(e * 2 * HALF, (e + 1) * 2 * HALF)
        packed = lift_ref[:, lanes]
        field_ref[:, lanes] = mm(packed, jnp.concatenate([high, high], 0)) + mm(packed[:, :HALF], low)

    def lane_blocks(at_rows):
        return [field_ref[at_rows, i * HALF : (i + 1) * HALF] for i in range(8)]

    def expose(s, total):
        at_rows = pl.ds(pl.multiple_of(s * rows, rows), rows)
        r0, i0, r1, i1, r2, i2, r3, i3 = lane_blocks(at_rows)
        real = [r0 + r2 + (r1 + r3), r0 - r2 - (i1 - i3), r0 + r2 - (r1 + r3), r0 - r2 + (i1 - i3)]
        imag = [i0 + i2 + (i1 + i3), i0 - i2 + (r1 - r3), i0 + i2 - (i1 + i3), i0 - i2 - (r1 - r3)]
        out = []
        for q in range(4):
            field_ref[at_rows, 2 * q * HALF : (2 * q + 1) * HALF] = real[q]
            field_ref[at_rows, (2 * q + 1) * HALF : (2 * q + 2) * HALF] = imag[q]
            out.append(total[q] + share_ref[s] * (real[q] * real[q] + imag[q] * imag[q]))
        return tuple(out)

    coarse = lax.fori_loop(0, sources, expose, (jnp.zeros((rows, HALF), f32),) * 4)
    spread = spread_high_ref[...], spread_low_ref[...]
    quarter = COARSE // 4
    spread = [tuple(t[at : at + n] for t in spread) for at, n in ((0, quarter), (quarter, quarter), (2 * quarter, 2 * quarter))]
    i0, i1, i2, i3 = coarse
    even, odd = i0 + i2, i1 + i3
    a, b = i0 - i2, i1 - i3
    e = mm3(pieces(even + odd), spread[0])
    f = mm3(pieces(even - odd), spread[1])
    rs = mm3(pieces(jnp.concatenate([jnp.concatenate([a, -b], 1), jnp.concatenate([b, a], 1)], 0)), spread[2])
    up, down = e + f, e - f
    r, t = rs[:rows], rs[rows:]
    fine = target_ref.shape[1] // 4
    slopes = []
    squares = jnp.zeros((rows, fine), f32)
    for q, intensity in enumerate((up + r, down + t, up - r, down - t)):
        resist = 1.0 / (1.0 + jnp.exp(-steepness * (intensity - threshold)))
        misfit = resist - target_ref[:, q * fine : (q + 1) * fine].astype(f32)
        slopes.append((2.0 * steepness) * misfit * resist * (1.0 - resist))
        squares = squares + misfit * misfit
    s0, s1, s2, s3 = slopes
    even, odd = s0 + s2, s1 + s3
    de = mm3(pieces(even + odd), spread[0], NT)
    df = mm3(pieces(even - odd), spread[1], NT)
    x = mm3(pieces(jnp.concatenate([s0 - s2, s1 - s3], 0)), spread[2], NT)
    da = x[:rows, :quarter] + x[rows:, quarter:]
    db = x[rows:, :quarter] - x[:rows, quarter:]
    up, down = de + df, de - df
    slope_c = [up + da, down + db, up - da, down - db]

    def lane_sum(a):
        a = jnp.sum(a, 0, keepdims=True)
        total = a[:, :128]
        for i in range(1, a.shape[1] // 128):
            total = total + a[:, i * 128 : (i + 1) * 128]
        return total

    sums_ref[...] = jnp.zeros(sums_ref.shape, f32)
    sums_ref[8:9, :] = lane_sum(squares)
    for ref in (pull_p_ref, pull_m_ref):
        ref[...] = jnp.zeros(ref.shape, f32)

    def push(s, carry):
        at_rows = pl.ds(pl.multiple_of(s * rows, rows), rows)
        blocks = lane_blocks(at_rows)
        bright = jnp.zeros((rows, HALF), f32)
        real, imag = [], []
        for q in range(4):
            re, im = blocks[2 * q], blocks[2 * q + 1]
            bright = bright + (re * re + im * im) * slope_c[q]
            factor = (2.0 * norming * share_ref[s]) * slope_c[q]
            real.append(factor * re)
            imag.append(factor * im)
        sums_ref[pl.ds(16 + s, 1), :] = jnp.sum(bright, 0, keepdims=True)
        er, ei, fr, fi = real[0] + real[2], imag[0] + imag[2], real[1] + real[3], imag[1] + imag[3]
        ar, ai, br, bi = real[0] - real[2], imag[0] - imag[2], real[1] - real[3], imag[1] - imag[3]
        turned = [er + fr, ei + fi, ar + bi, ai - br, er - fr, ei - fi, ar - bi, ai + br]
        for i, value in enumerate(turned):
            high, low = pieces(value)
            back_high_ref[at_rows, i * HALF : (i + 1) * HALF] = high
            back_low_ref[at_rows, i * HALF : (i + 1) * HALF] = low
        return carry

    lax.fori_loop(0, sources, push, 0)
    for e, (high, low) in enumerate(field_tables):
        lanes = slice(e * 2 * HALF, (e + 1) * 2 * HALF)
        both = mm(back_high_ref[:, lanes], jnp.concatenate([high, low], 0), NT)
        settled_ref[:, e * HALF : (e + 1) * HALF] = (
            both[:, :HALF] + both[:, HALF:] + mm(back_low_ref[:, lanes], high, NT)
        )

    def pull(s, carry):
        at_rows = pl.ds(pl.multiple_of(s * rows, rows), rows)
        settled = [settled_ref[at_rows, e * HALF : (e + 1) * HALF] for e in range(4)]
        arrays = [
            place(lambda i: (settled[(i + 1) % 4 if k < 2 else (3 - i) % 4], k)) for k in range(4)
        ]
        for pull_ref, table_ref, passed, at in zip(
            (pull_p_ref, pull_m_ref), (local_pt_ref, local_mt_ref), passes(s), (0, 2)
        ):
            high, low = pieces(jnp.concatenate(arrays[at : at + 2], 0))
            out = mm(table_ref[...], jnp.concatenate([high, low, high], 0))
            pull_ref[...] += out * jnp.concatenate([passed, passed], 0)
        return carry

    lax.fori_loop(0, sources, pull, 0)
    plus = pull_p_ref[...]
    minus = pull_m_ref[...]
    y_real = jnp.zeros((owners, rows), f32)
    y_imag = jnp.zeros((owners, rows), f32)
    for m, (c, n) in enumerate(turns_of):
        real = plus[m * owners : (m + 1) * owners, HALF - 1 :]
        imag = plus[K + m * owners : K + (m + 1) * owners, HALF - 1 :]
        y_real = y_real + (real * c - imag * n)
        y_imag = y_imag + (real * n + imag * c)
    level = mm3(turn, pieces(jnp.concatenate([y_real, -y_imag], 0)))
    sums = jnp.sum(sums_ref[...].T, 0, keepdims=True)
    lane = lane_index((owners, 128))
    level = jnp.concatenate([level] * 4, 1)
    tail = jnp.where(lane // rows == 1, level, sums)
    edge = jnp.concatenate([minus[:1], minus[K : K + 1], jnp.zeros((6, HALF), f32)], 0).T
    for j in range(2):
        for part in range(2):
            tail = jnp.where(lane == 2 * j + part, edge[j * owners : (j + 1) * owners, part : part + 1], tail)
    total = jnp.where(lane_index(plus.shape) == HALF - 1, 0.0, plus)
    total = total + jnp.where(row_index(plus.shape) % K == 0, 0.0, minus)
    total = total.T
    row = jnp.concatenate([total[:owners], total[owners:], tail], 1)
    low, high = row[:ring], row[ring:]
    out_mine_ref[...] = jnp.where(first_core, low, high).reshape(out_mine_ref.shape)
    out_theirs_ref[...] = jnp.where(first_core, high, low).reshape(out_theirs_ref.shape)


def owner_kernel(in_ref, high_ref, low_ref, cos_ref, sin_ref, out_ref, sums_ref):
    total = jnp.sum(in_ref[...], 0)
    tail = total[:, 4 * K :]
    sums_ref[...] = tail
    owners = HALF // 2
    rows = cos_ref.shape[1] // 4
    quantities = [total[:, q * K : (q + 1) * K] for q in range(4)]
    columns = jnp.concatenate(quantities + [jnp.zeros((4, K), f32)], 0).T
    lane = lane_index((owners, 4 * rows))
    where = lane // rows
    z = jnp.zeros((owners, 4 * rows), f32)
    for m in range(5):
        cos, sin = twiddle(cos_ref, sin_ref, m)
        if m < 4:
            part = columns[m * owners : (m + 1) * owners]
            cols = [part[:, q : q + 1] for q in range(4)]
        else:
            top = row_index((owners, 1)) == 0
            cols = [jnp.where(top, tail[:, q : q + 1], 0.0) for q in range(4)]
        straight = jnp.where(where == 0, cols[0], jnp.where(where == 1, cols[1], jnp.where(where == 2, cols[2], cols[3])))
        crossed = jnp.where(where == 0, -cols[1], jnp.where(where == 1, cols[0], jnp.where(where == 2, -cols[3], cols[2])))
        z = z + straight * cos + crossed * sin
    out = mm3((high_ref[...], low_ref[...]), pieces(jnp.concatenate([z, -swapped(z, rows)], 0)))
    out_ref[...] = out.reshape(out_ref.shape)


def grad_kernel(in_ref, sums_ref, share_ref, group_ref, high_ref, low_ref, out_ref, loss_ref, group_out_ref):
    rows, length = out_ref.shape
    quarter = length // 4
    owners = in_ref.shape[0]
    a = in_ref[...].reshape(owners, 4 * rows)
    odd_row = row_index((owners, rows)) % 2 == 1
    none = jnp.zeros((owners, rows), f32)
    real0, imag0, real1, imag1 = (a[:, i * rows : (i + 1) * rows] for i in range(4))
    top = jnp.concatenate(
        [none, jnp.where(odd_row, real0, 0.0), jnp.where(odd_row, 0.0, real0), jnp.where(odd_row, 0.0, -imag0)], 1
    )
    top_sin = jnp.concatenate(
        [none, jnp.where(odd_row, -imag0, 0.0), jnp.where(odd_row, 0.0, -imag0), jnp.where(odd_row, 0.0, -real0)], 1
    )
    low = jnp.concatenate(
        [jnp.where(odd_row, real1, 0.0), none, jnp.where(odd_row, 0.0, real1), jnp.where(odd_row, 0.0, imag1)], 1
    )
    low_sin = jnp.concatenate(
        [jnp.where(odd_row, -imag1, 0.0), none, jnp.where(odd_row, 0.0, -imag1), jnp.where(odd_row, 0.0, real1)], 1
    )
    stack = jnp.concatenate([top, low, top_sin, low_sin], 0).T
    both = mm3(pieces(stack), (high_ref[...], low_ref[...]))
    sums = sums_ref[...]
    const = jnp.broadcast_to(sums, (8, 128)).T[rows : 2 * rows, :1]
    e = both[:rows] + const
    f = both[rows : 2 * rows]
    g = both[2 * rows : 3 * rows]
    h = both[3 * rows :]
    up, down = e + f, e - f
    out_ref[:, :quarter] = up + g
    out_ref[:, quarter : 2 * quarter] = down + h
    out_ref[:, 2 * quarter : 3 * quarter] = up - g
    out_ref[:, 3 * quarter :] = down - h
    norming = 1.0 / (length * length)
    loss_ref[...] = sums[:, 8:9] * norming
    share = share_ref[...]
    against = jnp.sum(share * sums, 1, keepdims=True)
    pull = share * (sums - against) * norming
    group_out_ref[...] = jnp.sum((group_ref[...] * pull).T, 0, keepdims=True)


def tables(rows, length, ring):
    owners = HALF // 2
    z = np.arange(ring)
    by_owner = np.stack([4 * z + c + 1 for c in range(2)], 1).reshape(-1)
    slots = np.concatenate([by_owner, by_owner + 2])
    cos, sin = turns(slots, np.arange(length // 4), length)
    row_table = np.concatenate([cos, sin], 0)
    cos, sin = turns(np.arange(owners), np.arange(owners), owners)
    dft = np.concatenate([cos, sin], 1)
    in_order = np.concatenate([2 * z, 2 * z + 1])
    turn = dft[in_order]
    across = np.concatenate([np.arange(owners), owners * np.arange(8) - HALF])
    cos, sin = turns(across, np.arange(rows), length)
    turning = np.tile(cos, (1, 4)).astype(np.float32), np.tile(sin, (1, 4)).astype(np.float32)
    samples = (length // COARSE) * np.arange(COARSE)
    lanes = np.concatenate([4 * z + g + 1 for g in range(4)])
    first = np.concatenate([lanes[:-1], [0]])
    cos_p, sin_p = turns(first, samples[: COARSE // 4], length)
    cos_m, sin_m = turns(lanes, samples[: COARSE // 4], length)
    field = []
    for e in range(4):
        p, m = (slice(g * ring, (g + 1) * ring) for g in groups_of(e))
        real = np.concatenate([cos_p[p], -sin_p[p], cos_m[m], -sin_m[m]], 0)
        imag = np.concatenate([sin_p[p], cos_p[p], -sin_m[m], -cos_m[m]], 0)
        field.append(np.concatenate([real, imag], 1))
    field = np.concatenate(field, 0)
    tones = np.arange(1, COARSE // 2 + 1)
    share = np.where(tones == COARSE // 2, 1.0, 2.0)
    pixels = np.arange(length)
    kernel = (1.0 + np.cos(2.0 * np.pi * (np.outer(pixels, tones) % length) / length) @ share) / COARSE
    near, fine = samples[: COARSE // 4, None], pixels[None, : length // 4]
    h0, h1, h2, h3 = (kernel[(fine + p * (length // 4) - near) % length] for p in range(4))
    spread = np.concatenate([(h0 + h1 + h2 + h3) / 4, (h0 - h1 + h2 - h3) / 4, (h0 - h2) / 2, (h1 - h3) / 2], 0)
    return host_pieces(row_table), host_pieces(dft), host_pieces(turn), turning, host_pieces(field), host_pieces(spread)


def call(kernel, out_shape, scratch=(), n_scalar=0, n_in=0, interpret=False, flops=0):
    vmem = pl.BlockSpec(memory_space=pltpu.VMEM)
    smem = pl.BlockSpec(memory_space=pltpu.SMEM)
    multi = isinstance(out_shape, (tuple, list))
    return pl.pallas_call(
        kernel,
        out_shape=out_shape,
        in_specs=[smem] * n_scalar + [vmem] * n_in,
        out_specs=[vmem] * len(out_shape) if multi else vmem,
        scratch_shapes=list(scratch),
        compiler_params=pltpu.CompilerParams(vmem_limit_bytes=56 * 1024 * 1024),
        interpret=interpret,
    )


def image_scratch(sources, rows):
    vmem = pltpu.VMEM
    return [
        vmem((2 * K, 2 * HALF), bf16),
        vmem((2 * K, 2 * HALF), bf16),
        vmem((sources * rows, 8 * HALF), bf16),
        vmem((sources * rows, 2 * COARSE), f32),
        vmem((sources * rows, 2 * COARSE), bf16),
        vmem((sources * rows, 2 * COARSE), bf16),
        vmem((sources * rows, 4 * HALF), f32),
        vmem((2 * K, HALF), f32),
        vmem((2 * K, HALF), f32),
        vmem((128, 128), f32),
    ]


INTERPRET = False


def on_device(mask_field, target_print, source_points, source_groups, group_logits, pupil_radius):
    rows, length = mask_field.shape
    ring = lax.axis_size(RING)
    pair = lax.axis_size(CORE)
    owners = ring * pair
    sources = source_points.shape[0]
    row_table, dft, turn, turning, field, spread = tables(rows, length, ring)
    device = lax.axis_index(SLAB)
    norming = 1.0 / (length * length)
    cutoff = pupil_radius[0]
    shifted = (source_points - GRID // 2) * cutoff // shift_scale
    shape = functools.partial(jax.ShapeDtypeStruct, dtype=f32)
    run = functools.partial(call, interpret=INTERPRET)

    def swap_all(parcels, axes):
        return lax.all_to_all(parcels, axes, split_axis=0, concat_axis=0, tiled=True)

    parcels, own_sums = run(rows_kernel, (shape((owners, 1, 4 * rows)), shape((1, 128))), n_in=3)(mask_field, *row_table)
    arrived = swap_all(parcels, SLAB)
    piece = run(columns_kernel, shape((ring, 1, PARCEL)), n_in=6)(arrived, own_sums, *dft, *turning)
    around = swap_all(piece, RING)
    theirs = lax.ppermute(around, CORE, [(i, (i + 1) % pair) for i in range(pair)])

    onehot = (source_groups[:, None] == jnp.arange(NG, dtype=jnp.int32)[None, :]).astype(f32)
    weights = jnp.exp(jnp.sum(onehot * group_logits[None, :], 1))
    total_weight = jnp.sum(weights)
    weight_share = weights / total_weight
    across = jnp.arange(K, dtype=jnp.int32) - HALF
    across_m = jnp.where(across == -HALF, HALF, across)
    here = device * rows + jnp.arange(rows, dtype=jnp.int32)

    def local(freq):
        angle = jnp.mod(here[:, None] * freq[None, :], length).astype(f32) * (2.0 * np.pi / length)
        c, s = jnp.cos(angle), jnp.sin(angle)
        table = jnp.concatenate([jnp.concatenate([c, -s], 1), jnp.concatenate([s, c], 1)], 0)
        rounded = lax.reduce_precision(table, 8, 7)
        high, low = rounded.astype(bf16), (table - rounded).astype(bf16)
        return jnp.concatenate([high, low], 0), jnp.concatenate([high.T, high.T, low.T], 1)

    local_p, local_pt = local(across)
    local_m, local_mt = local(across_m)
    mine, theirs = run(
        image_kernel,
        (shape((ring, 1, PARCEL)),) * 2,
        n_scalar=4,
        n_in=15,
        scratch=image_scratch(sources, rows),
    )(
        shifted,
        weight_share,
        pupil_radius,
        lax.axis_index(CORE).reshape(1),
        around,
        theirs,
        *turn,
        *turning,
        local_p,
        local_m,
        local_pt,
        local_mt,
        *field,
        *spread,
        target_print,
    )
    mine = mine + lax.ppermute(theirs, CORE, [(i, (i + 1) % pair) for i in range(pair)])
    mine = swap_all(mine, RING)
    parcels, sums = run(owner_kernel, (shape((owners, 1, 4 * rows)), shape((1, 128))), n_in=5)(mine, *dft, *turning)
    arrived = swap_all(parcels, SLAB)
    share_row = jnp.zeros((1, 128), f32).at[0, 16 : 16 + sources].set(weight_share)
    group_rows = jnp.zeros((NG, 128), f32).at[:, 16 : 16 + sources].set(onehot.T)
    mask_grad, loss_value, group_grad = run(
        grad_kernel, (shape((rows, length)), shape((1, 1)), shape((1, NG))), n_in=6
    )(arrived, sums, share_row, group_rows, *row_table)
    return (loss_value.reshape(1), mask_grad, group_grad.reshape(NG))


def solution(mesh):
    cores = 2
    ring = mesh.shape["slab"] // cores
    split = Mesh(mesh.devices.reshape(mesh.shape["clip"], ring, cores), CLIP_SLAB)
    return jax.shard_map(
        on_device,
        mesh=split,
        in_specs=(
            P(CLIP_SLAB, None),
            P(CLIP_SLAB, None),
            P("clip", None),
            P("clip"),
            P("clip"),
            P("clip"),
        ),
        out_specs=(P("clip"), P(CLIP_SLAB, None), P("clip")),
        check_vma=False,
    )
```

```python
import functools

import numpy as np
import jax
import jax.numpy as jnp
from jax import lax
from jax.experimental import pallas as pl
from jax.experimental.pallas import tpu as pltpu
from jax.sharding import Mesh
from jax.sharding import PartitionSpec as P

K = 256
HALF = K // 2
GRID = 61
NG = 8
COARSE = 2 * K
PARCEL = 9 * 128
RING = "slab_0"
CORE = "slab_1"
SLAB = (RING, CORE)
CLIP_SLAB = ("clip", RING, CORE)

steepness = 8.0
threshold = 0.3
shift_scale = 45

f32 = jnp.float32
bf16 = jnp.bfloat16
NN = (((1,), (0,)), ((), ()))
NT = (((1,), (1,)), ((), ()))
TN = (((0,), (0,)), ((), ()))


def mm(a, b, dims=NN):
    return lax.dot_general(a, b, dims, preferred_element_type=f32)


def pieces(a):
    high = a.astype(bf16)
    return high, (a - high.astype(f32)).astype(bf16)


def mm3(a, b, dims=NN):
    return mm(a[0], b[0], dims) + mm(a[1], b[0], dims) + mm(a[0], b[1], dims)


def host_pieces(table):
    high = table.astype(np.float32).astype(jnp.bfloat16)
    low = (table - high.astype(np.float64)).astype(np.float32).astype(jnp.bfloat16)
    return np.asarray(high), np.asarray(low)


def turns(left, right, length):
    angle = 2.0 * np.pi * (np.outer(left, right) % length) / length
    return np.cos(angle), np.sin(angle)


def groups_of(e):
    return (e - 1) % 4, (3 - e) % 4


def lane_index(shape):
    return lax.broadcasted_iota(jnp.int32, shape, len(shape) - 1)


def row_index(shape):
    return lax.broadcasted_iota(jnp.int32, shape, 0)


def swapped(a, rows):
    lanes = a.shape[1]
    first = (lane_index(a.shape) // rows) % 2 == 0
    return jnp.where(first, pltpu.roll(a, lanes - rows, 1), -pltpu.roll(a, rows, 1))


def twiddle(cos_ref, sin_ref, m):
    owners = cos_ref.shape[0] - 8
    cos, sin = cos_ref[:owners], sin_ref[:owners]
    cos_m, sin_m = cos_ref[owners + m : owners + m + 1], sin_ref[owners + m : owners + m + 1]
    return cos * cos_m - sin * sin_m, sin * cos_m + cos * sin_m


def rows_kernel(mask_ref, high_ref, low_ref, out_ref, sums_ref):
    rows, length = mask_ref.shape
    quarter = length // 4
    m0, m1, m2, m3 = (mask_ref[:, q * quarter : (q + 1) * quarter] for q in range(4))
    even, odd = m0 + m2, m1 + m3
    stack = jnp.concatenate([even + odd, even - odd, m0 - m2, m1 - m3], 0)
    stack = pieces(stack)
    both = mm3((high_ref[...], low_ref[...]), stack, NT)
    cos, sin = both[:HALF], both[HALF:]
    c0, c2, ca, cb = (cos[:, i * rows : (i + 1) * rows] for i in range(4))
    s0, s2, sa, sb = (sin[:, i * rows : (i + 1) * rows] for i in range(4))
    owners = HALF // 2
    odd_row = row_index((owners, rows)) % 2 == 1
    lo, hi = slice(0, owners), slice(owners, HALF)
    ones = jnp.ones((8, quarter), bf16)
    sums_ref[...] = (mm(ones, stack[0], NT) + mm(ones, stack[1], NT))[:1]
    parcels = jnp.concatenate(
        [
            jnp.where(odd_row, c2[lo], ca[lo] - sb[lo]),
            jnp.where(odd_row, -s2[lo], -sa[lo] - cb[lo]),
            jnp.where(odd_row, c0[hi], ca[hi] + sb[hi]),
            jnp.where(odd_row, -s0[hi], cb[hi] - sa[hi]),
        ],
        1,
    )
    out_ref[...] = parcels.reshape(out_ref.shape)


def local_kernel(
    cos_ref, sin_ref, kernel_ref, plus_ref, minus_ref, plus_t_ref, minus_t_ref, spread_high_ref, spread_low_ref, ready_ref
):
    cos = cos_ref[...]
    edge = lane_index(cos.shape) == 0
    for out_ref, out_t_ref, sin in (
        (plus_ref, plus_t_ref, sin_ref[...]),
        (minus_ref, minus_t_ref, jnp.where(edge, -sin_ref[...], sin_ref[...])),
    ):
        table = jnp.concatenate([jnp.concatenate([cos, -sin], 1), jnp.concatenate([sin, cos], 1)], 0)
        high, low = pieces(table)
        out_ref[...] = jnp.concatenate([high, low], 0)
        high, low = pieces(table.T)
        out_t_ref[...] = jnp.concatenate([high, high, low], 1)
    ready_ref[...] = cos[:8, :128]
    length = kernel_ref.shape[1]
    near, fine = COARSE // 4, length // 4
    at = pltpu.roll(
        jnp.broadcast_to(kernel_ref[...], (near, length)), 0, 1, stride=length // COARSE, stride_axis=0
    )
    h0, h1, h2, h3 = (at[:, p * fine : (p + 1) * fine] for p in range(4))
    even, odd = h0 + h2, h1 + h3
    for i, table in enumerate(((even + odd) / 4, (even - odd) / 4, (h0 - h2) / 2, (h1 - h3) / 2)):
        high, low = pieces(table)
        spread_high_ref[i * near : (i + 1) * near] = high
        spread_low_ref[i * near : (i + 1) * near] = low


def columns_kernel(in_ref, own_sums_ref, dft_high_ref, dft_low_ref, cos_ref, sin_ref, ready_ref, piece_ref):
    owners, _, lanes = in_ref.shape
    rows = lanes // 4
    a = in_ref[...].reshape(owners, lanes)
    z = mm3((dft_high_ref[...], dft_low_ref[...]), pieces(jnp.concatenate([a, swapped(a, rows)], 0)))
    turned = swapped(z, rows)
    blocks = []
    for m in range(5):
        cos, sin = twiddle(cos_ref, sin_ref, m)
        blocks.append(z * cos + turned * sin)
    high, low = pieces(jnp.concatenate(blocks, 0))
    pick = (row_index((8, lanes)) == lane_index((8, lanes)) // rows).astype(f32).astype(bf16)
    sums = mm(pick, high, NT) + mm(pick, low, NT)
    copies = piece_ref.shape[0]
    lane = lane_index((1, 128))
    tail = jnp.where(lane // rows == 1, pltpu.roll(own_sums_ref[...], rows, 1), 0.0)
    for q in range(4):
        tail = jnp.where(lane == q, sums[q : q + 1, K : K + 1], tail)
    row = jnp.concatenate([sums[q : q + 1, :K] for q in range(4)] + [tail], 1)
    piece_ref[...] = jnp.broadcast_to(row.reshape(1, 1, PARCEL), (copies, 1, PARCEL))


def image_kernel(
    shift_ref,
    share_ref,
    radius_ref,
    core_ref,
    mine_ref,
    theirs_ref,
    turn_high_ref,
    turn_low_ref,
    cos_ref,
    sin_ref,
    local_p_ref,
    local_m_ref,
    local_pt_ref,
    local_mt_ref,
    field_high_ref,
    field_low_ref,
    spread_high_ref,
    spread_low_ref,
    target_ref,
    out_mine_ref,
    out_theirs_ref,
    plus_ref,
    minus_ref,
    lift_ref,
    field_ref,
    back_high_ref,
    back_low_ref,
    settled_ref,
    pull_p_ref,
    pull_m_ref,
    sums_ref,
):
    sources = shift_ref.shape[0]
    rows = target_ref.shape[0]
    half = 2 * rows
    norming = 1.0 / (target_ref.shape[1] * target_ref.shape[1])
    radius_sq = radius_ref[0] * radius_ref[0]
    first_core = core_ref[0] == 0
    ring = mine_ref.shape[0]
    mine = mine_ref[...].reshape(ring, PARCEL)
    theirs = theirs_ref[...].reshape(ring, PARCEL)
    wide = jnp.concatenate([jnp.where(first_core, mine, theirs), jnp.where(first_core, theirs, mine)], 0)
    body = jnp.concatenate([wide[:, : 2 * K], wide[:, 2 * K : 4 * K]], 0)
    spectrum = body.T
    tail = wide[:, 4 * K :].T
    turn = turn_high_ref[...], turn_low_ref[...]
    owners = 2 * ring
    z = mm3(turn, pieces(wide[:, 4 * K + rows : 4 * K + 2 * rows]), TN)
    z_real, z_imag = z[:owners], -z[owners:]
    turns_of = [tuple(t[:, :rows] for t in twiddle(cos_ref, sin_ref, m)) for m in range(4)]
    zero = [
        jnp.concatenate([jnp.sum(z_real * c + z_imag * n, 1, keepdims=True) for c, n in turns_of], 0),
        jnp.concatenate([jnp.sum(z_imag * c - z_real * n, 1, keepdims=True) for c, n in turns_of], 0),
    ]
    lane = lane_index((1, HALF))
    frequency = 4 * (lane % ring) + lane // ring + 1
    last = lane == HALF - 1
    frequency_p = jnp.where(last, 0, frequency)
    across = row_index((K, 1)) - HALF
    across_m = jnp.where(across == -HALF, HALF, across)
    last_col = lane_index((K, HALF)) == HALF - 1
    first_row = row_index((K, HALF)) == 0
    for part in range(2):
        block = spectrum[part * K : (part + 1) * K]
        plus = jnp.where(last_col, zero[part], block)
        edge = jnp.concatenate([tail[part : part + 1], tail[2 + part : 3 + part]], 1)
        minus = jnp.where(first_row, edge, block)
        for ref, value in ((plus_ref, plus), (minus_ref, minus)):
            high, low = pieces(value)
            ref[part * K : (part + 1) * K, :HALF] = high
            ref[part * K : (part + 1) * K, HALF:] = low

    def passes(s):
        s0 = shift_ref[s, 0]
        s1 = shift_ref[s, 1]
        a = across + s0
        b = frequency_p + s1
        plus = a * a <= radius_sq - b * b
        a = s0 - across_m
        b = s1 - frequency
        minus = a * a <= radius_sq - b * b
        return jnp.where(plus, 1.0, 0.0), jnp.where(minus, 1.0, 0.0)

    block = HALF // 4
    in_block = [lane_index((rows, HALF)) // block == i for i in range(4)]

    def place(choose):
        out = None
        for i in range(4):
            value, group = choose(i)
            value = pltpu.roll(value, (i - group) % 4 * block, 1) if i != group else value
            out = value if out is None else jnp.where(in_block[i], value, out)
        return out

    def lift(s, carry):
        parts = []
        for spec_ref, table_ref, passed in zip((plus_ref, minus_ref), (local_p_ref, local_m_ref), passes(s)):
            passed = passed.astype(bf16)
            passed = jnp.concatenate([passed, passed], 0)
            passed = jnp.concatenate([passed, passed], 1)
            out = mm(table_ref[...], spec_ref[...] * passed)
            out = (out[:half, :HALF] + out[half:, :HALF] + out[:half, HALF:]) * norming
            parts += [out[:rows], out[rows:]]
        at_rows = pl.ds(pl.multiple_of(s * rows, rows), rows)
        for e in range(4):
            groups = groups_of(e)
            high, low = pieces(place(lambda i: (parts[i], groups[i // 2])))
            lift_ref[at_rows, e * 2 * HALF : e * 2 * HALF + HALF] = high
            lift_ref[at_rows, e * 2 * HALF + HALF : (e + 1) * 2 * HALF] = low
        return carry

    lax.fori_loop(0, sources, lift, 0, unroll=16)
    field_tables = [
        (field_high_ref[e * HALF : (e + 1) * HALF], field_low_ref[e * HALF : (e + 1) * HALF]) for e in range(4)
    ]
    for e, (high, low) in enumerate(field_tables):
        lanes = slice(e * 2 * HALF, (e + 1) * 2 * HALF)
        packed = lift_ref[:, lanes]
        field_ref[:, lanes] = mm(packed, jnp.concatenate([high, high], 0)) + mm(packed[:, :HALF], low)

    def lane_blocks(at_rows):
        return [field_ref[at_rows, i * HALF : (i + 1) * HALF] for i in range(8)]

    def expose(s, total):
        at_rows = pl.ds(pl.multiple_of(s * rows, rows), rows)
        r0, i0, r1, i1, r2, i2, r3, i3 = lane_blocks(at_rows)
        real = [r0 + r2 + (r1 + r3), r0 - r2 - (i1 - i3), r0 + r2 - (r1 + r3), r0 - r2 + (i1 - i3)]
        imag = [i0 + i2 + (i1 + i3), i0 - i2 + (r1 - r3), i0 + i2 - (i1 + i3), i0 - i2 - (r1 - r3)]
        out = []
        for q in range(4):
            field_ref[at_rows, 2 * q * HALF : (2 * q + 1) * HALF] = real[q]
            field_ref[at_rows, (2 * q + 1) * HALF : (2 * q + 2) * HALF] = imag[q]
            out.append(total[q] + share_ref[s] * (real[q] * real[q] + imag[q] * imag[q]))
        return tuple(out)

    coarse = lax.fori_loop(0, sources, expose, (jnp.zeros((rows, HALF), f32),) * 4, unroll=2)
    spread = spread_high_ref[...], spread_low_ref[...]
    quarter = COARSE // 4
    spread = [tuple(t[at : at + n] for t in spread) for at, n in ((0, quarter), (quarter, quarter), (2 * quarter, 2 * quarter))]
    i0, i1, i2, i3 = coarse
    even, odd = i0 + i2, i1 + i3
    a, b = i0 - i2, i1 - i3
    e = mm3(pieces(even + odd), spread[0])
    f = mm3(pieces(even - odd), spread[1])
    rs = mm3(pieces(jnp.concatenate([jnp.concatenate([a, -b], 1), jnp.concatenate([b, a], 1)], 0)), spread[2])
    up, down = e + f, e - f
    r, t = rs[:rows], rs[rows:]
    fine = target_ref.shape[1] // 4
    slopes = []
    squares = jnp.zeros((rows, fine), f32)
    for q, intensity in enumerate((up + r, down + t, up - r, down - t)):
        resist = 1.0 / (1.0 + jnp.exp(-steepness * (intensity - threshold)))
        misfit = resist - target_ref[:, q * fine : (q + 1) * fine].astype(f32)
        slopes.append((2.0 * steepness) * misfit * resist * (1.0 - resist))
        squares = squares + misfit * misfit
    s0, s1, s2, s3 = slopes
    even, odd = s0 + s2, s1 + s3
    de = mm3(pieces(even + odd), spread[0], NT)
    df = mm3(pieces(even - odd), spread[1], NT)
    x = mm3(pieces(jnp.concatenate([s0 - s2, s1 - s3], 0)), spread[2], NT)
    da = x[:rows, :quarter] + x[rows:, quarter:]
    db = x[rows:, :quarter] - x[:rows, quarter:]
    up, down = de + df, de - df
    slope_c = [up + da, down + db, up - da, down - db]

    def lane_sum(a):
        a = jnp.sum(a, 0, keepdims=True)
        total = a[:, :128]
        for i in range(1, a.shape[1] // 128):
            total = total + a[:, i * 128 : (i + 1) * 128]
        return total

    sums_ref[...] = jnp.zeros(sums_ref.shape, f32)
    sums_ref[8:9, :] = lane_sum(squares)
    for ref in (pull_p_ref, pull_m_ref):
        ref[...] = jnp.zeros(ref.shape, f32)

    def push(s, carry):
        at_rows = pl.ds(pl.multiple_of(s * rows, rows), rows)
        blocks = lane_blocks(at_rows)
        bright = jnp.zeros((rows, HALF), f32)
        real, imag = [], []
        for q in range(4):
            re, im = blocks[2 * q], blocks[2 * q + 1]
            bright = bright + (re * re + im * im) * slope_c[q]
            factor = (2.0 * norming * share_ref[s]) * slope_c[q]
            real.append(factor * re)
            imag.append(factor * im)
        sums_ref[pl.ds(16 + s, 1), :] = jnp.sum(bright, 0, keepdims=True)
        er, ei, fr, fi = real[0] + real[2], imag[0] + imag[2], real[1] + real[3], imag[1] + imag[3]
        ar, ai, br, bi = real[0] - real[2], imag[0] - imag[2], real[1] - real[3], imag[1] - imag[3]
        turned = [er + fr, ei + fi, ar + bi, ai - br, er - fr, ei - fi, ar - bi, ai + br]
        for i, value in enumerate(turned):
            high, low = pieces(value)
            back_high_ref[at_rows, i * HALF : (i + 1) * HALF] = high
            back_low_ref[at_rows, i * HALF : (i + 1) * HALF] = low
        return carry

    lax.fori_loop(0, sources, push, 0, unroll=2)
    for e, (high, low) in enumerate(field_tables):
        lanes = slice(e * 2 * HALF, (e + 1) * 2 * HALF)
        both = mm(back_high_ref[:, lanes], jnp.concatenate([high, low], 0), NT)
        settled_ref[:, e * HALF : (e + 1) * HALF] = (
            both[:, :HALF] + both[:, HALF:] + mm(back_low_ref[:, lanes], high, NT)
        )

    def pull(s, carry):
        at_rows = pl.ds(pl.multiple_of(s * rows, rows), rows)
        settled = [settled_ref[at_rows, e * HALF : (e + 1) * HALF] for e in range(4)]
        arrays = [
            place(lambda i: (settled[(i + 1) % 4 if k < 2 else (3 - i) % 4], k)) for k in range(4)
        ]
        for pull_ref, table_ref, passed, at in zip(
            (pull_p_ref, pull_m_ref), (local_pt_ref, local_mt_ref), passes(s), (0, 2)
        ):
            high, low = pieces(jnp.concatenate(arrays[at : at + 2], 0))
            out = mm(table_ref[...], jnp.concatenate([high, low, high], 0))
            pull_ref[...] += out * jnp.concatenate([passed, passed], 0)
        return carry

    lax.fori_loop(0, sources, pull, 0, unroll=16)
    plus = pull_p_ref[...]
    minus = pull_m_ref[...]
    y_real = jnp.zeros((owners, rows), f32)
    y_imag = jnp.zeros((owners, rows), f32)
    for m, (c, n) in enumerate(turns_of):
        real = plus[m * owners : (m + 1) * owners, HALF - 1 :]
        imag = plus[K + m * owners : K + (m + 1) * owners, HALF - 1 :]
        y_real = y_real + (real * c - imag * n)
        y_imag = y_imag + (real * n + imag * c)
    level = mm3(turn, pieces(jnp.concatenate([y_real, -y_imag], 0)))
    sums = jnp.sum(sums_ref[...].T, 0, keepdims=True)
    lane = lane_index((owners, 128))
    level = jnp.concatenate([level] * 4, 1)
    tail = jnp.where(lane // rows == 1, level, sums)
    edge = jnp.concatenate([minus[:1], minus[K : K + 1], jnp.zeros((6, HALF), f32)], 0).T
    for j in range(2):
        for part in range(2):
            tail = jnp.where(lane == 2 * j + part, edge[j * owners : (j + 1) * owners, part : part + 1], tail)
    total = jnp.where(lane_index(plus.shape) == HALF - 1, 0.0, plus)
    total = total + jnp.where(row_index(plus.shape) % K == 0, 0.0, minus)
    total = total.T
    row = jnp.concatenate([total[:owners], total[owners:], tail], 1)
    low, high = row[:ring], row[ring:]
    out_mine_ref[...] = jnp.where(first_core, low, high).reshape(out_mine_ref.shape)
    out_theirs_ref[...] = jnp.where(first_core, high, low).reshape(out_theirs_ref.shape)


def owner_kernel(in_ref, high_ref, low_ref, cos_ref, sin_ref, out_ref, sums_ref):
    total = jnp.sum(in_ref[...], 0)
    tail = total[:, 4 * K :]
    sums_ref[...] = tail
    owners = HALF // 2
    rows = cos_ref.shape[1] // 4
    quantities = [total[:, q * K : (q + 1) * K] for q in range(4)]
    columns = jnp.concatenate(quantities + [jnp.zeros((4, K), f32)], 0).T
    lane = lane_index((owners, 4 * rows))
    where = lane // rows
    z = jnp.zeros((owners, 4 * rows), f32)
    for m in range(5):
        cos, sin = twiddle(cos_ref, sin_ref, m)
        if m < 4:
            part = columns[m * owners : (m + 1) * owners]
            cols = [part[:, q : q + 1] for q in range(4)]
        else:
            top = row_index((owners, 1)) == 0
            cols = [jnp.where(top, tail[:, q : q + 1], 0.0) for q in range(4)]
        straight = jnp.where(where == 0, cols[0], jnp.where(where == 1, cols[1], jnp.where(where == 2, cols[2], cols[3])))
        crossed = jnp.where(where == 0, -cols[1], jnp.where(where == 1, cols[0], jnp.where(where == 2, -cols[3], cols[2])))
        z = z + straight * cos + crossed * sin
    out = mm3((high_ref[...], low_ref[...]), pieces(jnp.concatenate([z, -swapped(z, rows)], 0)))
    out_ref[...] = out.reshape(out_ref.shape)


def grad_kernel(in_ref, sums_ref, share_ref, group_ref, high_ref, low_ref, out_ref, loss_ref, group_out_ref):
    rows, length = out_ref.shape
    quarter = length // 4
    owners = in_ref.shape[0]
    a = in_ref[...].reshape(owners, 4 * rows)
    odd_row = row_index((owners, rows)) % 2 == 1
    none = jnp.zeros((owners, rows), f32)
    real0, imag0, real1, imag1 = (a[:, i * rows : (i + 1) * rows] for i in range(4))
    top = jnp.concatenate(
        [none, jnp.where(odd_row, real0, 0.0), jnp.where(odd_row, 0.0, real0), jnp.where(odd_row, 0.0, -imag0)], 1
    )
    top_sin = jnp.concatenate(
        [none, jnp.where(odd_row, -imag0, 0.0), jnp.where(odd_row, 0.0, -imag0), jnp.where(odd_row, 0.0, -real0)], 1
    )
    low = jnp.concatenate(
        [jnp.where(odd_row, real1, 0.0), none, jnp.where(odd_row, 0.0, real1), jnp.where(odd_row, 0.0, imag1)], 1
    )
    low_sin = jnp.concatenate(
        [jnp.where(odd_row, -imag1, 0.0), none, jnp.where(odd_row, 0.0, -imag1), jnp.where(odd_row, 0.0, real1)], 1
    )
    stack = jnp.concatenate([top, low, top_sin, low_sin], 0).T
    both = mm3(pieces(stack), (high_ref[...], low_ref[...]))
    sums = sums_ref[...]
    const = jnp.broadcast_to(sums, (8, 128)).T[rows : 2 * rows, :1]
    e = both[:rows] + const
    f = both[rows : 2 * rows]
    g = both[2 * rows : 3 * rows]
    h = both[3 * rows :]
    up, down = e + f, e - f
    out_ref[:, :quarter] = up + g
    out_ref[:, quarter : 2 * quarter] = down + h
    out_ref[:, 2 * quarter : 3 * quarter] = up - g
    out_ref[:, 3 * quarter :] = down - h
    norming = 1.0 / (length * length)
    loss_ref[...] = sums[:, 8:9] * norming
    share = share_ref[...]
    against = jnp.sum(share * sums, 1, keepdims=True)
    pull = share * (sums - against) * norming
    group_out_ref[...] = jnp.sum((group_ref[...] * pull).T, 0, keepdims=True)


def tables(rows, length, ring):
    owners = HALF // 2
    z = np.arange(ring)
    by_owner = np.stack([4 * z + c + 1 for c in range(2)], 1).reshape(-1)
    slots = np.concatenate([by_owner, by_owner + 2])
    cos, sin = turns(slots, np.arange(length // 4), length)
    row_table = np.concatenate([cos, sin], 0)
    cos, sin = turns(np.arange(owners), np.arange(owners), owners)
    dft = np.concatenate([cos, sin], 1)
    in_order = np.concatenate([2 * z, 2 * z + 1])
    turn = dft[in_order]
    across = np.concatenate([np.arange(owners), owners * np.arange(8) - HALF])
    cos, sin = turns(across, np.arange(rows), length)
    turning = np.tile(cos, (1, 4)).astype(np.float32), np.tile(sin, (1, 4)).astype(np.float32)
    samples = (length // COARSE) * np.arange(COARSE)
    lanes = np.concatenate([4 * z + g + 1 for g in range(4)])
    first = np.concatenate([lanes[:-1], [0]])
    cos_p, sin_p = turns(first, samples[: COARSE // 4], length)
    cos_m, sin_m = turns(lanes, samples[: COARSE // 4], length)
    field = []
    for e in range(4):
        p, m = (slice(g * ring, (g + 1) * ring) for g in groups_of(e))
        real = np.concatenate([cos_p[p], -sin_p[p], cos_m[m], -sin_m[m]], 0)
        imag = np.concatenate([sin_p[p], cos_p[p], -sin_m[m], -cos_m[m]], 0)
        field.append(np.concatenate([real, imag], 1))
    field = np.concatenate(field, 0)
    tones = np.arange(1, COARSE // 2 + 1)
    share = np.where(tones == COARSE // 2, 1.0, 2.0)
    pixels = np.arange(length)
    kernel = (1.0 + np.cos(2.0 * np.pi * (np.outer(pixels, tones) % length) / length) @ share) / COARSE
    spread = kernel.reshape(1, length).astype(np.float32)
    return host_pieces(row_table), host_pieces(dft), host_pieces(turn), turning, host_pieces(field), spread


def call(kernel, out_shape, scratch=(), n_scalar=0, n_in=0, mib=12, interpret=False):
    vmem = pl.BlockSpec(memory_space=pltpu.VMEM)
    smem = pl.BlockSpec(memory_space=pltpu.SMEM)
    multi = isinstance(out_shape, (tuple, list))
    return pl.pallas_call(
        kernel,
        out_shape=out_shape,
        in_specs=[smem] * n_scalar + [vmem] * n_in,
        out_specs=[vmem] * len(out_shape) if multi else vmem,
        scratch_shapes=list(scratch),
        compiler_params=pltpu.CompilerParams(vmem_limit_bytes=mib * 1024 * 1024),
        interpret=interpret,
    )


def image_scratch(sources, rows):
    vmem = pltpu.VMEM
    return [
        vmem((2 * K, 2 * HALF), bf16),
        vmem((2 * K, 2 * HALF), bf16),
        vmem((sources * rows, 8 * HALF), bf16),
        vmem((sources * rows, 2 * COARSE), f32),
        vmem((sources * rows, 2 * COARSE), bf16),
        vmem((sources * rows, 2 * COARSE), bf16),
        vmem((sources * rows, 4 * HALF), f32),
        vmem((2 * K, HALF), f32),
        vmem((2 * K, HALF), f32),
        vmem((128, 128), f32),
    ]


INTERPRET = False


def on_device(mask_field, target_print, source_points, source_groups, group_logits, pupil_radius):
    rows, length = mask_field.shape
    ring = lax.axis_size(RING)
    pair = lax.axis_size(CORE)
    owners = ring * pair
    sources = source_points.shape[0]
    row_table, dft, turn, turning, field, spread = tables(rows, length, ring)
    device = lax.axis_index(SLAB)
    norming = 1.0 / (length * length)
    cutoff = pupil_radius[0]
    shifted = (source_points - GRID // 2) * cutoff // shift_scale
    shape = functools.partial(jax.ShapeDtypeStruct, dtype=f32)
    run = functools.partial(call, interpret=INTERPRET)

    def swap_all(parcels, axes):
        return lax.all_to_all(parcels, axes, split_axis=0, concat_axis=0, tiled=True)

    parcels, own_sums = run(rows_kernel, (shape((owners, 1, 4 * rows)), shape((1, 128))), n_in=3)(mask_field, *row_table)
    arrived = swap_all(parcels, SLAB)
    across = jnp.arange(K, dtype=jnp.int32) - HALF
    here = device * rows + jnp.arange(rows, dtype=jnp.int32)
    angle = jnp.mod(here[:, None] * across[None, :], length).astype(f32) * (2.0 * np.pi / length)
    sizes = ((4 * rows, 2 * K),) * 2 + ((2 * K, 6 * rows),) * 2 + ((COARSE, length // 4),) * 2
    local_p, local_m, local_pt, local_mt, *spread, ready = run(
        local_kernel,
        tuple(jax.ShapeDtypeStruct(t, bf16) for t in sizes) + (shape((8, 128)),),
        n_in=3,
    )(jnp.cos(angle), jnp.sin(angle), spread)
    piece = run(columns_kernel, shape((ring, 1, PARCEL)), n_in=7)(arrived, own_sums, *dft, *turning, ready)
    around = swap_all(piece, RING)
    theirs = lax.ppermute(around, CORE, [(i, (i + 1) % pair) for i in range(pair)])

    onehot = (source_groups[:, None] == jnp.arange(NG, dtype=jnp.int32)[None, :]).astype(f32)
    weights = jnp.exp(jnp.sum(onehot * group_logits[None, :], 1))
    total_weight = jnp.sum(weights)
    weight_share = weights / total_weight
    mine, theirs = run(
        image_kernel,
        (shape((ring, 1, PARCEL)),) * 2,
        n_scalar=4,
        n_in=15,
        mib=28,
        scratch=image_scratch(sources, rows),
    )(
        shifted,
        weight_share,
        pupil_radius,
        lax.axis_index(CORE).reshape(1),
        around,
        theirs,
        *turn,
        *turning,
        local_p,
        local_m,
        local_pt,
        local_mt,
        *field,
        *spread,
        target_print,
    )
    mine = mine + lax.ppermute(theirs, CORE, [(i, (i + 1) % pair) for i in range(pair)])
    mine = swap_all(mine, RING)
    parcels, sums = run(owner_kernel, (shape((owners, 1, 4 * rows)), shape((1, 128))), n_in=5)(mine, *dft, *turning)
    arrived = swap_all(parcels, SLAB)
    share_row = jnp.zeros((1, 128), f32).at[0, 16 : 16 + sources].set(weight_share)
    group_rows = jnp.zeros((NG, 128), f32).at[:, 16 : 16 + sources].set(onehot.T)
    mask_grad, loss_value, group_grad = run(
        grad_kernel, (shape((rows, length)), shape((1, 1)), shape((1, NG))), n_in=6
    )(arrived, sums, share_row, group_rows, *row_table)
    return (loss_value.reshape(1), mask_grad, group_grad.reshape(NG))


def solution(mesh):
    cores = 2
    ring = mesh.shape["slab"] // cores
    split = Mesh(mesh.devices.reshape(mesh.shape["clip"], ring, cores), CLIP_SLAB)
    return jax.shard_map(
        on_device,
        mesh=split,
        in_specs=(
            P(CLIP_SLAB, None),
            P(CLIP_SLAB, None),
            P("clip", None),
            P("clip"),
            P("clip"),
            P("clip"),
        ),
        out_specs=(P("clip"), P(CLIP_SLAB, None), P("clip")),
        check_vma=False,
    )
```

```python
import functools

import numpy as np
import jax
import jax.numpy as jnp
from jax import lax
from jax.experimental import pallas as pl
from jax.experimental.pallas import tpu as pltpu
from jax.sharding import Mesh
from jax.sharding import PartitionSpec as P

K = 256
HALF = K // 2
GRID = 61
NG = 8
COARSE = 2 * K
FAR = 4
SPECTRA = K * K // 16
FAR_AXIS = "slab_0"
NEAR = "slab_1"
CORE = "slab_2"
SLAB = (FAR_AXIS, NEAR, CORE)
CLIP_SLAB = ("clip", *SLAB)

steepness = 8.0
threshold = 0.3
shift_scale = 45

f32 = jnp.float32
bf16 = jnp.bfloat16
NN = (((1,), (0,)), ((), ()))
NT = (((1,), (1,)), ((), ()))
TN = (((0,), (0,)), ((), ()))


def mm(a, b, dims=NN):
    return lax.dot_general(a, b, dims, preferred_element_type=f32)


def pieces(a):
    high = a.astype(bf16)
    return high, (a - high.astype(f32)).astype(bf16)


def mm3(a, b, dims=NN):
    return mm(a[0], b[0], dims) + mm(a[1], b[0], dims) + mm(a[0], b[1], dims)


def host_pieces(table):
    high = table.astype(np.float32).astype(jnp.bfloat16)
    low = (table - high.astype(np.float64)).astype(np.float32).astype(jnp.bfloat16)
    return np.asarray(high), np.asarray(low)


def turns(left, right, length):
    angle = 2.0 * np.pi * (np.outer(left, right) % length) / length
    return np.cos(angle), np.sin(angle)


def groups_of(e):
    return (e - 1) % 4, (3 - e) % 4


def lane_index(shape):
    return lax.broadcasted_iota(jnp.int32, shape, len(shape) - 1)


def row_index(shape):
    return lax.broadcasted_iota(jnp.int32, shape, 0)


def swapped(a, rows):
    lanes = a.shape[1]
    first = (lane_index(a.shape) // rows) % 2 == 0
    return jnp.where(first, pltpu.roll(a, lanes - rows, 1), -pltpu.roll(a, rows, 1))


def twiddle(cos_ref, sin_ref, m):
    owners = cos_ref.shape[0] - 8
    cos, sin = cos_ref[:owners], sin_ref[:owners]
    cos_m, sin_m = cos_ref[owners + m : owners + m + 1], sin_ref[owners + m : owners + m + 1]
    return cos * cos_m - sin * sin_m, sin * cos_m + cos * sin_m


def rows_kernel(mask_ref, high_ref, low_ref, out_ref):
    rows, length = mask_ref.shape
    quarter = length // 4
    m0, m1, m2, m3 = (mask_ref[:, q * quarter : (q + 1) * quarter] for q in range(4))
    even, odd = m0 + m2, m1 + m3
    stack = jnp.concatenate([even + odd, even - odd, m0 - m2, m1 - m3], 0)
    stack = pieces(stack)
    both = mm3((high_ref[...], low_ref[...]), stack, NT)
    cos, sin = both[:HALF], both[HALF:]
    c0, c2, ca, cb = (cos[:, i * rows : (i + 1) * rows] for i in range(4))
    s0, s2, sa, sb = (sin[:, i * rows : (i + 1) * rows] for i in range(4))
    ones = jnp.ones((8, quarter), bf16)
    sums = (mm(ones, stack[0], NT) + mm(ones, stack[1], NT))[:1, :rows]
    group = HALF // 4
    g0, g1, g2, g3 = (slice(g * group, (g + 1) * group) for g in range(4))
    real = [ca[g0] - sb[g0], c2[g1], ca[g2] + sb[g2], c0[g3]]
    imag = [-sa[g0] - cb[g0], -s2[g1], cb[g2] - sa[g2], -s0[g3]]
    owners = out_ref.shape[0] // FAR
    slots = group // owners
    blocks = []
    for re, im in zip(real, imag):
        for t in range(slots):
            blocks += [re[t * owners : (t + 1) * owners], im[t * owners : (t + 1) * owners]]
    blocks += [jnp.broadcast_to(sums, (owners, rows)), jnp.zeros((owners, 3 * rows), f32)]
    parcels = jnp.concatenate(blocks, 1)
    out_ref[...] = jnp.concatenate([parcels] * FAR, 0).reshape(out_ref.shape)


def local_kernel(
    cos_ref, sin_ref, kernel_ref, plus_ref, minus_ref, plus_t_ref, minus_t_ref, spread_high_ref, spread_low_ref, ready_ref
):
    cos = cos_ref[...]
    edge = lane_index(cos.shape) == 0
    for out_ref, out_t_ref, sin in (
        (plus_ref, plus_t_ref, sin_ref[...]),
        (minus_ref, minus_t_ref, jnp.where(edge, -sin_ref[...], sin_ref[...])),
    ):
        table = jnp.concatenate([jnp.concatenate([cos, -sin], 1), jnp.concatenate([sin, cos], 1)], 0)
        high, low = pieces(table)
        out_ref[...] = jnp.concatenate([high, low], 0)
        high, low = pieces(table.T)
        out_t_ref[...] = jnp.concatenate([high, high, low], 1)
    ready_ref[...] = cos[:8, :128]
    length = kernel_ref.shape[1]
    near, fine = COARSE // 4, length // 4
    at = pltpu.roll(
        jnp.broadcast_to(kernel_ref[...], (near, length)), 0, 1, stride=length // COARSE, stride_axis=0
    )
    h0, h1, h2, h3 = (at[:, p * fine : (p + 1) * fine] for p in range(4))
    even, odd = h0 + h2, h1 + h3
    for i, table in enumerate(((even + odd) / 4, (even - odd) / 4, (h0 - h2) / 2, (h1 - h3) / 2)):
        high, low = pieces(table)
        spread_high_ref[i * near : (i + 1) * near] = high
        spread_low_ref[i * near : (i + 1) * near] = low


def columns_kernel(in_ref, dft_high_ref, dft_low_ref, cos_ref, sin_ref, ready_ref, piece_ref):
    devices, _, lanes = in_ref.shape
    rows = cos_ref.shape[1] // 4
    lanes -= 4 * rows
    a = in_ref[...].reshape(devices, lanes + 4 * rows)[:, :lanes]
    z = mm3((dft_high_ref[...], dft_low_ref[...]), pieces(jnp.concatenate([a, swapped(a, rows)], 0)))
    turned = swapped(z, rows)
    blocks = []
    for m in range(5):
        cos, sin = (jnp.concatenate([t] * (lanes // (4 * rows)), 1) for t in twiddle(cos_ref, sin_ref, m))
        blocks.append(z * cos + turned * sin)
    high, low = pieces(jnp.concatenate(blocks, 0))
    count = lanes // rows
    pick = (row_index((count, lanes)) == lane_index((count, lanes)) // rows).astype(f32).astype(bf16)
    sums = mm(pick, high, NT) + mm(pick, low, NT)
    copies = piece_ref.shape[0]
    lane = lane_index((1, 128))
    tail = jnp.zeros((1, 128), f32)
    for q in range(count):
        tail = jnp.where(lane == q, sums[q : q + 1, K : K + 1], tail)
    row = jnp.concatenate([sums[q : q + 1, :K] for q in range(count)] + [tail], 1)
    piece_ref[...] = jnp.broadcast_to(row.reshape(1, 1, row.shape[1]), (copies, 1, row.shape[1]))


def image_kernel(
    shift_ref,
    share_ref,
    radius_ref,
    core_ref,
    mine_ref,
    theirs_ref,
    arrived_ref,
    dft_high_ref,
    dft_low_ref,
    turn_high_ref,
    turn_low_ref,
    cos_ref,
    sin_ref,
    local_p_ref,
    local_m_ref,
    local_pt_ref,
    local_mt_ref,
    field_high_ref,
    field_low_ref,
    spread_high_ref,
    spread_low_ref,
    target_ref,
    out_mine_ref,
    out_theirs_ref,
    plus_ref,
    minus_ref,
    lift_ref,
    field_ref,
    back_high_ref,
    back_low_ref,
    settled_ref,
    pull_p_ref,
    pull_m_ref,
    sums_ref,
):
    sources = shift_ref.shape[0]
    rows = target_ref.shape[0]
    half = 2 * rows
    norming = 1.0 / (target_ref.shape[1] * target_ref.shape[1])
    radius_sq = radius_ref[0] * radius_ref[0]
    first_core = core_ref[0] == 0
    near = mine_ref.shape[0]
    mine = mine_ref[...].reshape(near, SPECTRA + 128)
    theirs = theirs_ref[...].reshape(near, SPECTRA + 128)
    wide = jnp.concatenate([jnp.where(first_core, mine, theirs), jnp.where(first_core, theirs, mine)], 0)
    owners = 2 * near
    slots = HALF // owners
    body = jnp.concatenate([wide[:, t * 2 * K : (t + 1) * 2 * K] for t in range(slots)], 0)
    spectrum = body.T
    tail = [
        jnp.concatenate([wide[:, SPECTRA + 2 * t + part : SPECTRA + 2 * t + part + 1] for t in range(slots)], 0)
        for part in range(2)
    ]
    tail = jnp.concatenate(tail + [jnp.zeros((HALF, 6), f32)], 1).T
    devices = arrived_ref.shape[0]
    row_sums = arrived_ref[...].reshape(devices, arrived_ref.shape[2])[:, arrived_ref.shape[2] - 4 * rows :]
    z = mm3((dft_high_ref[...], dft_low_ref[...]), pieces(row_sums[:, :rows]), TN)
    z_real, z_imag = z[:devices], -z[devices:]
    turns_of = [tuple(t[:, :rows] for t in twiddle(cos_ref, sin_ref, m)) for m in range(4)]
    zero = [
        jnp.concatenate([jnp.sum(z_real * c + z_imag * n, 1, keepdims=True) for c, n in turns_of], 0),
        jnp.concatenate([jnp.sum(z_imag * c - z_real * n, 1, keepdims=True) for c, n in turns_of], 0),
    ]
    lane = lane_index((1, HALF))
    frequency = 4 * (lane % (HALF // 4)) + lane // (HALF // 4) + 1
    last = lane == HALF - 1
    frequency_p = jnp.where(last, 0, frequency)
    across = row_index((K, 1)) - HALF
    across_m = jnp.where(across == -HALF, HALF, across)
    last_col = lane_index((K, HALF)) == HALF - 1
    first_row = row_index((K, HALF)) == 0
    for part in range(2):
        block = spectrum[part * K : (part + 1) * K]
        plus = jnp.where(last_col, zero[part], block)
        minus = jnp.where(first_row, tail[part : part + 1], block)
        for ref, value in ((plus_ref, plus), (minus_ref, minus)):
            high, low = pieces(value)
            ref[part * K : (part + 1) * K, :HALF] = high
            ref[part * K : (part + 1) * K, HALF:] = low

    def passes(s):
        s0 = shift_ref[s, 0]
        s1 = shift_ref[s, 1]
        a = across + s0
        b = frequency_p + s1
        plus = a * a <= radius_sq - b * b
        a = s0 - across_m
        b = s1 - frequency
        minus = a * a <= radius_sq - b * b
        return jnp.where(plus, 1.0, 0.0), jnp.where(minus, 1.0, 0.0)

    block = HALF // 4
    in_block = [lane_index((rows, HALF)) // block == i for i in range(4)]

    def place(choose):
        out = None
        for i in range(4):
            value, group = choose(i)
            value = pltpu.roll(value, (i - group) % 4 * block, 1) if i != group else value
            out = value if out is None else jnp.where(in_block[i], value, out)
        return out

    def lift(s, carry):
        parts = []
        for spec_ref, table_ref, passed in zip((plus_ref, minus_ref), (local_p_ref, local_m_ref), passes(s)):
            passed = passed.astype(bf16)
            passed = jnp.concatenate([passed, passed], 0)
            passed = jnp.concatenate([passed, passed], 1)
            out = mm(table_ref[...], spec_ref[...] * passed)
            out = (out[:half, :HALF] + out[half:, :HALF] + out[:half, HALF:]) * norming
            parts += [out[:rows], out[rows:]]
        at_rows = pl.ds(pl.multiple_of(s * rows, rows), rows)
        for e in range(4):
            groups = groups_of(e)
            high, low = pieces(place(lambda i: (parts[i], groups[i // 2])))
            lift_ref[at_rows, e * 2 * HALF : e * 2 * HALF + HALF] = high
            lift_ref[at_rows, e * 2 * HALF + HALF : (e + 1) * 2 * HALF] = low
        return carry

    lax.fori_loop(0, sources, lift, 0, unroll=16)
    field_tables = [
        (field_high_ref[e * HALF : (e + 1) * HALF], field_low_ref[e * HALF : (e + 1) * HALF]) for e in range(4)
    ]
    for e, (high, low) in enumerate(field_tables):
        lanes = slice(e * 2 * HALF, (e + 1) * 2 * HALF)
        packed = lift_ref[:, lanes]
        field_ref[:, lanes] = mm(packed, jnp.concatenate([high, high], 0)) + mm(packed[:, :HALF], low)

    def lane_blocks(at_rows):
        return [field_ref[at_rows, i * HALF : (i + 1) * HALF] for i in range(8)]

    def expose(s, total):
        at_rows = pl.ds(pl.multiple_of(s * rows, rows), rows)
        r0, i0, r1, i1, r2, i2, r3, i3 = lane_blocks(at_rows)
        real = [r0 + r2 + (r1 + r3), r0 - r2 - (i1 - i3), r0 + r2 - (r1 + r3), r0 - r2 + (i1 - i3)]
        imag = [i0 + i2 + (i1 + i3), i0 - i2 + (r1 - r3), i0 + i2 - (i1 + i3), i0 - i2 - (r1 - r3)]
        out = []
        for q in range(4):
            field_ref[at_rows, 2 * q * HALF : (2 * q + 1) * HALF] = real[q]
            field_ref[at_rows, (2 * q + 1) * HALF : (2 * q + 2) * HALF] = imag[q]
            out.append(total[q] + share_ref[s] * (real[q] * real[q] + imag[q] * imag[q]))
        return tuple(out)

    coarse = lax.fori_loop(0, sources, expose, (jnp.zeros((rows, HALF), f32),) * 4, unroll=2)
    spread = spread_high_ref[...], spread_low_ref[...]
    quarter = COARSE // 4
    spread = [tuple(t[at : at + n] for t in spread) for at, n in ((0, quarter), (quarter, quarter), (2 * quarter, 2 * quarter))]
    i0, i1, i2, i3 = coarse
    even, odd = i0 + i2, i1 + i3
    a, b = i0 - i2, i1 - i3
    e = mm3(pieces(even + odd), spread[0])
    f = mm3(pieces(even - odd), spread[1])
    rs = mm3(pieces(jnp.concatenate([jnp.concatenate([a, -b], 1), jnp.concatenate([b, a], 1)], 0)), spread[2])
    up, down = e + f, e - f
    r, t = rs[:rows], rs[rows:]
    fine = target_ref.shape[1] // 4
    slopes = []
    squares = jnp.zeros((rows, fine), f32)
    for q, intensity in enumerate((up + r, down + t, up - r, down - t)):
        resist = 1.0 / (1.0 + jnp.exp(-steepness * (intensity - threshold)))
        misfit = resist - target_ref[:, q * fine : (q + 1) * fine].astype(f32)
        slopes.append((2.0 * steepness) * misfit * resist * (1.0 - resist))
        squares = squares + misfit * misfit
    s0, s1, s2, s3 = slopes
    even, odd = s0 + s2, s1 + s3
    de = mm3(pieces(even + odd), spread[0], NT)
    df = mm3(pieces(even - odd), spread[1], NT)
    x = mm3(pieces(jnp.concatenate([s0 - s2, s1 - s3], 0)), spread[2], NT)
    da = x[:rows, :quarter] + x[rows:, quarter:]
    db = x[rows:, :quarter] - x[:rows, quarter:]
    up, down = de + df, de - df
    slope_c = [up + da, down + db, up - da, down - db]

    def lane_sum(a):
        a = jnp.sum(a, 0, keepdims=True)
        total = a[:, :128]
        for i in range(1, a.shape[1] // 128):
            total = total + a[:, i * 128 : (i + 1) * 128]
        return total

    sums_ref[...] = jnp.zeros(sums_ref.shape, f32)
    sums_ref[80:81, :] = lane_sum(squares)
    for ref in (pull_p_ref, pull_m_ref):
        ref[...] = jnp.zeros(ref.shape, f32)

    def push(s, carry):
        at_rows = pl.ds(pl.multiple_of(s * rows, rows), rows)
        blocks = lane_blocks(at_rows)
        bright = jnp.zeros((rows, HALF), f32)
        real, imag = [], []
        for q in range(4):
            re, im = blocks[2 * q], blocks[2 * q + 1]
            bright = bright + (re * re + im * im) * slope_c[q]
            factor = (2.0 * norming * share_ref[s]) * slope_c[q]
            real.append(factor * re)
            imag.append(factor * im)
        sums_ref[pl.ds(64 + s, 1), :] = jnp.sum(bright, 0, keepdims=True)
        er, ei, fr, fi = real[0] + real[2], imag[0] + imag[2], real[1] + real[3], imag[1] + imag[3]
        ar, ai, br, bi = real[0] - real[2], imag[0] - imag[2], real[1] - real[3], imag[1] - imag[3]
        turned = [er + fr, ei + fi, ar + bi, ai - br, er - fr, ei - fi, ar - bi, ai + br]
        for i, value in enumerate(turned):
            high, low = pieces(value)
            back_high_ref[at_rows, i * HALF : (i + 1) * HALF] = high
            back_low_ref[at_rows, i * HALF : (i + 1) * HALF] = low
        return carry

    lax.fori_loop(0, sources, push, 0, unroll=2)
    for e, (high, low) in enumerate(field_tables):
        lanes = slice(e * 2 * HALF, (e + 1) * 2 * HALF)
        both = mm(back_high_ref[:, lanes], jnp.concatenate([high, low], 0), NT)
        settled_ref[:, e * HALF : (e + 1) * HALF] = (
            both[:, :HALF] + both[:, HALF:] + mm(back_low_ref[:, lanes], high, NT)
        )

    def pull(s, carry):
        at_rows = pl.ds(pl.multiple_of(s * rows, rows), rows)
        settled = [settled_ref[at_rows, e * HALF : (e + 1) * HALF] for e in range(4)]
        arrays = [
            place(lambda i: (settled[(i + 1) % 4 if k < 2 else (3 - i) % 4], k)) for k in range(4)
        ]
        for pull_ref, table_ref, passed, at in zip(
            (pull_p_ref, pull_m_ref), (local_pt_ref, local_mt_ref), passes(s), (0, 2)
        ):
            high, low = pieces(jnp.concatenate(arrays[at : at + 2], 0))
            out = mm(table_ref[...], jnp.concatenate([high, low, high], 0))
            pull_ref[...] += out * jnp.concatenate([passed, passed], 0)
        return carry

    lax.fori_loop(0, sources, pull, 0, unroll=16)
    plus = pull_p_ref[...]
    minus = pull_m_ref[...]
    y_real = jnp.zeros((devices, rows), f32)
    y_imag = jnp.zeros((devices, rows), f32)
    for m, (c, n) in enumerate(turns_of):
        real = plus[m * devices : (m + 1) * devices, HALF - 1 :]
        imag = plus[K + m * devices : K + (m + 1) * devices, HALF - 1 :]
        y_real = y_real + (real * c - imag * n)
        y_imag = y_imag + (real * n + imag * c)
    turn = turn_high_ref[...], turn_low_ref[...]
    level = mm3(turn, pieces(jnp.concatenate([y_real, -y_imag], 0)))
    level = jnp.concatenate([level[f * owners : (f + 1) * owners] for f in range(FAR)], 1)
    sums = jnp.sum(sums_ref[...].T, 0, keepdims=True)
    lane = lane_index((owners, 128))
    tail = jnp.broadcast_to(sums, (owners, 128))
    edge = jnp.concatenate([minus[:1], minus[K : K + 1], jnp.zeros((6, HALF), f32)], 0).T
    for t in range(slots):
        for part in range(2):
            tail = jnp.where(lane == 2 * t + part, edge[t * owners : (t + 1) * owners, part : part + 1], tail)
    total = jnp.where(lane_index(plus.shape) == HALF - 1, 0.0, plus)
    total = total + jnp.where(row_index(plus.shape) % K == 0, 0.0, minus)
    total = total.T
    row = jnp.concatenate([total[t * owners : (t + 1) * owners] for t in range(slots)] + [tail, level], 1)
    low, high = row[:near], row[near:]
    out_mine_ref[...] = jnp.where(first_core, low, high).reshape(out_mine_ref.shape)
    out_theirs_ref[...] = jnp.where(first_core, high, low).reshape(out_theirs_ref.shape)


def owner_kernel(own_ref, in_ref, high_ref, low_ref, cos_ref, sin_ref, out_ref):
    total = jnp.sum(in_ref[...], 0)
    tail = total[:, SPECTRA : SPECTRA + 128]
    devices = out_ref.shape[0]
    rows = cos_ref.shape[1] // 4
    count = SPECTRA // K
    owners = devices // FAR
    columns = jnp.concatenate([total[:, q * K : (q + 1) * K] for q in range(count)], 0).T
    where = lane_index((devices, 4 * rows)) // rows
    top = row_index((devices, 1)) == 0
    z = [jnp.zeros((devices, 4 * rows), f32)] * (count // 4)
    for m in range(5):
        cos, sin = twiddle(cos_ref, sin_ref, m)
        for i in range(count // 4):
            if m < 4:
                part = columns[m * devices : (m + 1) * devices]
                cols = [part[:, q : q + 1] for q in range(4 * i, 4 * i + 4)]
            else:
                cols = [jnp.where(top, tail[:, q : q + 1], 0.0) for q in range(4 * i, 4 * i + 4)]
            straight = jnp.where(where < 2, jnp.where(where == 0, cols[0], cols[1]), jnp.where(where == 2, cols[2], cols[3]))
            crossed = jnp.where(where < 2, jnp.where(where == 0, -cols[1], cols[0]), jnp.where(where == 2, -cols[3], cols[2]))
            z[i] = z[i] + straight * cos + crossed * sin
    z = jnp.concatenate(z, 1)
    out = mm3((high_ref[...], low_ref[...]), pieces(jnp.concatenate([z, -swapped(z, rows)], 0)))
    device = row_index((devices, rows))
    level = jnp.zeros((devices, rows), f32)
    for f in range(FAR):
        at = SPECTRA + 128 + f * rows
        level = jnp.where(device // owners == f, total[:, at : at + rows], level)
    level = jnp.where(device % owners == own_ref[0], level, 0.0)
    extra = jnp.concatenate([level, jnp.broadcast_to(tail[:, rows:] * (1.0 / owners), (devices, 3 * rows))], 1)
    out_ref[...] = jnp.concatenate([out, extra], 1).reshape(out_ref.shape)


def grad_kernel(in_ref, share_ref, group_ref, high_ref, low_ref, out_ref, loss_ref, group_out_ref):
    rows, length = out_ref.shape
    quarter = length // 4
    devices, _, lanes = in_ref.shape
    owners = devices // FAR
    a = in_ref[...].reshape(devices, lanes)
    parts = [a[f * owners : (f + 1) * owners] for f in range(FAR)]
    a = (parts[0] + parts[1]) + (parts[2] + parts[3])
    none = jnp.zeros((owners, rows), f32)
    slots = HALF // owners
    by_cos, by_sin = [], []
    for t in range(slots):
        re, im = a[:, 2 * t * rows : (2 * t + 1) * rows], a[:, (2 * t + 1) * rows : (2 * t + 2) * rows]
        group = t * owners // (HALF // 4)
        by_cos += [jnp.concatenate(([none, none, re, -im], [none, re, none, none], [none, none, re, im], [re, none, none, none])[group], 1)]
        by_sin += [jnp.concatenate(([none, none, -im, -re], [none, -im, none, none], [none, none, -im, re], [-im, none, none, none])[group], 1)]
    stack = jnp.concatenate(by_cos + by_sin, 0).T
    both = mm3(pieces(stack), (high_ref[...], low_ref[...]))
    sums = jnp.sum(a[:, 2 * slots * rows :], 0, keepdims=True)
    const = jnp.broadcast_to(sums, (8, 128)).T[:rows, :1]
    e = both[:rows] + const
    f = both[rows : 2 * rows]
    g = both[2 * rows : 3 * rows]
    h = both[3 * rows :]
    up, down = e + f, e - f
    out_ref[:, :quarter] = up + g
    out_ref[:, quarter : 2 * quarter] = down + h
    out_ref[:, 2 * quarter : 3 * quarter] = up - g
    out_ref[:, 3 * quarter :] = down - h
    norming = 1.0 / (length * length)
    loss_ref[...] = sums[:, 80:81] * norming
    share = share_ref[...]
    against = jnp.sum(share * sums, 1, keepdims=True)
    pull = share * (sums - against) * norming
    group_out_ref[...] = jnp.sum((group_ref[...] * pull).T, 0, keepdims=True)


def tables(rows, length, near):
    devices = 2 * near * FAR
    owner = np.arange(2 * near)
    t = np.arange(HALF // len(owner))[:, None]
    place = t * len(owner) + (owner % 2) * near + owner // 2
    slots = (4 * (place % (HALF // 4)) + place // (HALF // 4) + 1).reshape(-1)
    cos, sin = turns(slots, np.arange(length // 4), length)
    row_table = np.concatenate([cos, sin], 0)
    cos, sin = turns(np.arange(devices), np.arange(devices), devices)
    dft = np.concatenate([cos, sin], 1)
    n = np.arange(near)
    in_order = np.concatenate([2 * near * f + 2 * n + c for f in range(FAR) for c in range(2)])
    turn = dft[in_order]
    across = np.concatenate([np.arange(devices), devices * np.arange(8) - HALF])
    cos, sin = turns(across, np.arange(rows), length)
    turning = np.tile(cos, (1, 4)).astype(np.float32), np.tile(sin, (1, 4)).astype(np.float32)
    samples = (length // COARSE) * np.arange(COARSE)
    group = HALF // 4
    lanes = np.concatenate([4 * np.arange(group) + g + 1 for g in range(4)])
    first = np.concatenate([lanes[:-1], [0]])
    cos_p, sin_p = turns(first, samples[: COARSE // 4], length)
    cos_m, sin_m = turns(lanes, samples[: COARSE // 4], length)
    field = []
    for e in range(4):
        p, m = (slice(g * group, (g + 1) * group) for g in groups_of(e))
        real = np.concatenate([cos_p[p], -sin_p[p], cos_m[m], -sin_m[m]], 0)
        imag = np.concatenate([sin_p[p], cos_p[p], -sin_m[m], -cos_m[m]], 0)
        field.append(np.concatenate([real, imag], 1))
    field = np.concatenate(field, 0)
    tones = np.arange(1, COARSE // 2 + 1)
    share = np.where(tones == COARSE // 2, 1.0, 2.0)
    pixels = np.arange(length)
    kernel = (1.0 + np.cos(2.0 * np.pi * (np.outer(pixels, tones) % length) / length) @ share) / COARSE
    spread = kernel.reshape(1, length).astype(np.float32)
    return host_pieces(row_table), host_pieces(dft), host_pieces(turn), turning, host_pieces(field), spread


def call(kernel, out_shape, scratch=(), n_scalar=0, n_in=0, mib=12, interpret=False):
    vmem = pl.BlockSpec(memory_space=pltpu.VMEM)
    smem = pl.BlockSpec(memory_space=pltpu.SMEM)
    multi = isinstance(out_shape, (tuple, list))
    return pl.pallas_call(
        kernel,
        out_shape=out_shape,
        in_specs=[smem] * n_scalar + [vmem] * n_in,
        out_specs=[vmem] * len(out_shape) if multi else vmem,
        scratch_shapes=list(scratch),
        compiler_params=pltpu.CompilerParams(vmem_limit_bytes=mib * 1024 * 1024),
        interpret=interpret,
    )


def image_scratch(sources, rows):
    vmem = pltpu.VMEM
    return [
        vmem((2 * K, 2 * HALF), bf16),
        vmem((2 * K, 2 * HALF), bf16),
        vmem((sources * rows, 8 * HALF), bf16),
        vmem((sources * rows, 2 * COARSE), f32),
        vmem((sources * rows, 2 * COARSE), bf16),
        vmem((sources * rows, 2 * COARSE), bf16),
        vmem((sources * rows, 4 * HALF), f32),
        vmem((2 * K, HALF), f32),
        vmem((2 * K, HALF), f32),
        vmem((128, 128), f32),
    ]


INTERPRET = False


def on_device(mask_field, target_print, source_points, source_groups, group_logits, pupil_radius):
    rows, length = mask_field.shape
    near = lax.axis_size(NEAR)
    pair = lax.axis_size(CORE)
    devices = FAR * near * pair
    sources = source_points.shape[0]
    row_table, dft, turn, turning, field, spread = tables(rows, length, near)
    device = lax.axis_index(SLAB)
    norming = 1.0 / (length * length)
    cutoff = pupil_radius[0]
    shifted = (source_points - GRID // 2) * cutoff // shift_scale
    shape = functools.partial(jax.ShapeDtypeStruct, dtype=f32)
    run = functools.partial(call, interpret=INTERPRET)

    def swap_all(parcels, axes):
        return lax.all_to_all(parcels, axes, split_axis=0, concat_axis=0, tiled=True)

    width = 2 * HALF // (near * pair) * rows + 4 * rows
    parcels = run(rows_kernel, shape((devices, 1, width)), n_in=3, mib=56)(mask_field, *row_table)
    arrived = swap_all(parcels, SLAB)
    across = jnp.arange(K, dtype=jnp.int32) - HALF
    here = device * rows + jnp.arange(rows, dtype=jnp.int32)
    angle = jnp.mod(here[:, None] * across[None, :], length).astype(f32) * (2.0 * np.pi / length)
    sizes = ((4 * rows, 2 * K),) * 2 + ((2 * K, 6 * rows),) * 2 + ((COARSE, length // 4),) * 2
    local_p, local_m, local_pt, local_mt, *spread, ready = run(
        local_kernel,
        tuple(jax.ShapeDtypeStruct(t, bf16) for t in sizes) + (shape((8, 128)),),
        n_in=3,
    )(jnp.cos(angle), jnp.sin(angle), spread)
    piece = run(columns_kernel, shape((near, 1, SPECTRA + 128)), n_in=6)(arrived, *dft, *turning, ready)
    around = swap_all(piece, NEAR)
    theirs = lax.ppermute(around, CORE, [(i, (i + 1) % pair) for i in range(pair)])

    onehot = (source_groups[:, None] == jnp.arange(NG, dtype=jnp.int32)[None, :]).astype(f32)
    weights = jnp.exp(jnp.sum(onehot * group_logits[None, :], 1))
    total_weight = jnp.sum(weights)
    weight_share = weights / total_weight
    mine, theirs = run(
        image_kernel,
        (shape((near, 1, SPECTRA + 256)),) * 2,
        n_scalar=4,
        n_in=18,
        mib=28,
        scratch=image_scratch(sources, rows),
    )(
        shifted,
        weight_share,
        pupil_radius,
        lax.axis_index(CORE).reshape(1),
        around,
        theirs,
        arrived,
        *dft,
        *turn,
        *turning,
        local_p,
        local_m,
        local_pt,
        local_mt,
        *field,
        *spread,
        target_print,
    )
    mine = mine + lax.ppermute(theirs, CORE, [(i, (i + 1) % pair) for i in range(pair)])
    mine = swap_all(mine, NEAR)
    own = (lax.axis_index(NEAR) * pair + lax.axis_index(CORE)).reshape(1)
    parcels = run(owner_kernel, shape((devices, 1, width)), n_scalar=1, n_in=5)(own, mine, *dft, *turning)
    arrived = swap_all(parcels, SLAB)
    share_row = jnp.zeros((1, 128), f32).at[0, 64 : 64 + sources].set(weight_share)
    group_rows = jnp.zeros((NG, 128), f32).at[:, 64 : 64 + sources].set(onehot.T)
    mask_grad, loss_value, group_grad = run(
        grad_kernel, (shape((rows, length)), shape((1, 1)), shape((1, NG))), n_in=5
    )(arrived, share_row, group_rows, *row_table)
    return (loss_value.reshape(1), mask_grad, group_grad.reshape(NG))


def solution(mesh):
    cores = 2
    near = mesh.shape["slab"] // cores // FAR
    split = Mesh(mesh.devices.reshape(mesh.shape["clip"], FAR, near, cores), CLIP_SLAB)
    return jax.shard_map(
        on_device,
        mesh=split,
        in_specs=(
            P(CLIP_SLAB, None),
            P(CLIP_SLAB, None),
            P("clip", None),
            P("clip"),
            P("clip"),
            P("clip"),
        ),
        out_specs=(P("clip"), P(CLIP_SLAB, None), P("clip")),
        check_vma=False,
    )
```

```python
import functools

import numpy as np
import jax
import jax.numpy as jnp
from jax import lax
from jax.experimental import pallas as pl
from jax.experimental.pallas import tpu as pltpu
from jax.sharding import Mesh
from jax.sharding import PartitionSpec as P

K = 256
HALF = K // 2
GRID = 61
NG = 8
COARSE = 2 * K
FAR = 4
SPECTRA = K * K // 16
FAR_AXIS = "slab_0"
NEAR = "slab_1"
CORE = "slab_2"
SLAB = (FAR_AXIS, NEAR, CORE)
CLIP_SLAB = ("clip", *SLAB)

steepness = 8.0
threshold = 0.3
shift_scale = 45

f32 = jnp.float32
bf16 = jnp.bfloat16
NN = (((1,), (0,)), ((), ()))
NT = (((1,), (1,)), ((), ()))
TN = (((0,), (0,)), ((), ()))


def mm(a, b, dims=NN):
    return lax.dot_general(a, b, dims, preferred_element_type=f32)


def pieces(a):
    high = a.astype(bf16)
    return high, (a - high.astype(f32)).astype(bf16)


def mm3(a, b, dims=NN):
    return mm(a[0], b[0], dims) + mm(a[1], b[0], dims) + mm(a[0], b[1], dims)


def host_pieces(table):
    high = table.astype(np.float32).astype(jnp.bfloat16)
    low = (table - high.astype(np.float64)).astype(np.float32).astype(jnp.bfloat16)
    return np.asarray(high), np.asarray(low)


def turns(left, right, length):
    angle = 2.0 * np.pi * (np.outer(left, right) % length) / length
    return np.cos(angle), np.sin(angle)


def groups_of(e):
    return (e - 1) % 4, (3 - e) % 4


def lane_index(shape):
    return lax.broadcasted_iota(jnp.int32, shape, len(shape) - 1)


def row_index(shape):
    return lax.broadcasted_iota(jnp.int32, shape, 0)


def swapped(a, rows):
    lanes = a.shape[1]
    first = (lane_index(a.shape) // rows) % 2 == 0
    return jnp.where(first, pltpu.roll(a, lanes - rows, 1), -pltpu.roll(a, rows, 1))


def twiddle(cos_ref, sin_ref, m):
    owners = cos_ref.shape[0] - 8
    cos, sin = cos_ref[:owners], sin_ref[:owners]
    cos_m, sin_m = cos_ref[owners + m : owners + m + 1], sin_ref[owners + m : owners + m + 1]
    return cos * cos_m - sin * sin_m, sin * cos_m + cos * sin_m


def rows_kernel(mask_ref, high_ref, low_ref, out_ref):
    rows, length = mask_ref.shape
    quarter = length // 4
    m0, m1, m2, m3 = (mask_ref[:, q * quarter : (q + 1) * quarter] for q in range(4))
    even, odd = m0 + m2, m1 + m3
    stack = jnp.concatenate([even + odd, even - odd, m0 - m2, m1 - m3], 0)
    stack = pieces(stack)
    both = mm3((high_ref[...], low_ref[...]), stack, NT)
    cos, sin = both[:HALF], both[HALF:]
    c0, c2, ca, cb = (cos[:, i * rows : (i + 1) * rows] for i in range(4))
    s0, s2, sa, sb = (sin[:, i * rows : (i + 1) * rows] for i in range(4))
    ones = jnp.ones((8, quarter), bf16)
    sums = (mm(ones, stack[0], NT) + mm(ones, stack[1], NT))[:1, :rows]
    group = HALF // 4
    g0, g1, g2, g3 = (slice(g * group, (g + 1) * group) for g in range(4))
    real = [ca[g0] - sb[g0], c2[g1], ca[g2] + sb[g2], c0[g3]]
    imag = [-sa[g0] - cb[g0], -s2[g1], cb[g2] - sa[g2], -s0[g3]]
    owners = out_ref.shape[0] // FAR
    slots = group // owners
    blocks = []
    for re, im in zip(real, imag):
        for t in range(slots):
            blocks += [re[t * owners : (t + 1) * owners], im[t * owners : (t + 1) * owners]]
    blocks += [jnp.broadcast_to(sums, (owners, rows)), jnp.zeros((owners, 3 * rows), f32)]
    parcels = jnp.concatenate(blocks, 1)
    out_ref[...] = jnp.concatenate([parcels] * FAR, 0).reshape(out_ref.shape)


def local_kernel(
    cos_ref, sin_ref, kernel_ref, plus_ref, minus_ref, plus_t_ref, minus_t_ref, spread_high_ref, spread_low_ref, ready_ref
):
    cos = cos_ref[...]
    edge = lane_index(cos.shape) == 0
    for out_ref, out_t_ref, sin in (
        (plus_ref, plus_t_ref, sin_ref[...]),
        (minus_ref, minus_t_ref, jnp.where(edge, -sin_ref[...], sin_ref[...])),
    ):
        table = jnp.concatenate([jnp.concatenate([cos, -sin], 1), jnp.concatenate([sin, cos], 1)], 0)
        high, low = pieces(table)
        out_ref[...] = jnp.concatenate([high, low], 0)
        high, low = pieces(table.T)
        out_t_ref[...] = jnp.concatenate([high, high, low], 1)
    ready_ref[...] = cos[:8, :128]
    length = kernel_ref.shape[1]
    near, fine = COARSE // 4, length // 4
    at = pltpu.roll(
        jnp.broadcast_to(kernel_ref[...], (near, length)), 0, 1, stride=length // COARSE, stride_axis=0
    )
    h0, h1, h2, h3 = (at[:, p * fine : (p + 1) * fine] for p in range(4))
    even, odd = h0 + h2, h1 + h3
    for i, table in enumerate(((even + odd) / 4, (even - odd) / 4, (h0 - h2) / 2, (h1 - h3) / 2)):
        high, low = pieces(table)
        spread_high_ref[i * near : (i + 1) * near] = high
        spread_low_ref[i * near : (i + 1) * near] = low


def columns_kernel(in_ref, dft_high_ref, dft_low_ref, cos_ref, sin_ref, ready_ref, share_ref, piece_ref):
    devices, _, lanes = in_ref.shape
    rows = cos_ref.shape[1] // 4
    lanes -= 4 * rows
    a = in_ref[...].reshape(devices, lanes + 4 * rows)[:, :lanes]
    z = mm3((dft_high_ref[...], dft_low_ref[...]), pieces(jnp.concatenate([a, swapped(a, rows)], 0)))
    turned = swapped(z, rows)
    blocks = []
    for m in range(5):
        cos, sin = (jnp.concatenate([t] * (lanes // (4 * rows)), 1) for t in twiddle(cos_ref, sin_ref, m))
        blocks.append(z * cos + turned * sin)
    high, low = pieces(jnp.concatenate(blocks, 0))
    count = lanes // rows
    pick = (row_index((count, lanes)) == lane_index((count, lanes)) // rows).astype(f32).astype(bf16)
    sums = mm(pick, high, NT) + mm(pick, low, NT)
    copies = piece_ref.shape[0]
    lane = lane_index((1, 128))
    tail = jnp.zeros((1, 128), f32)
    for q in range(count):
        tail = jnp.where(lane == q, sums[q : q + 1, K : K + 1], tail)
    row = jnp.concatenate([sums[q : q + 1, :K] for q in range(count)] + [tail], 1)
    piece_ref[...] = jnp.broadcast_to(row.reshape(1, 1, row.shape[1]), (copies, 1, row.shape[1]))


def image_kernel(
    shift_ref,
    share_ref,
    radius_ref,
    core_ref,
    mine_ref,
    theirs_ref,
    arrived_ref,
    dft_high_ref,
    dft_low_ref,
    turn_high_ref,
    turn_low_ref,
    cos_ref,
    sin_ref,
    local_p_ref,
    local_m_ref,
    local_pt_ref,
    local_mt_ref,
    field_high_ref,
    field_low_ref,
    spread_high_ref,
    spread_low_ref,
    target_ref,
    out_mine_ref,
    out_theirs_ref,
    plus_ref,
    minus_ref,
    lift_ref,
    field_ref,
    back_high_ref,
    back_low_ref,
    settled_ref,
    pull_p_ref,
    pull_m_ref,
    sums_ref,
):
    sources = shift_ref.shape[0]
    rows = target_ref.shape[0]
    half = 2 * rows
    norming = 1.0 / (target_ref.shape[1] * target_ref.shape[1])
    radius_sq = radius_ref[0] * radius_ref[0]
    first_core = core_ref[0] == 0
    near = mine_ref.shape[0]
    mine = mine_ref[...].reshape(near, SPECTRA + 128)
    theirs = theirs_ref[...].reshape(near, SPECTRA + 128)
    wide = jnp.concatenate([jnp.where(first_core, mine, theirs), jnp.where(first_core, theirs, mine)], 0)
    owners = 2 * near
    slots = HALF // owners
    body = jnp.concatenate([wide[:, t * 2 * K : (t + 1) * 2 * K] for t in range(slots)], 0)
    spectrum = body.T
    tail = [
        jnp.concatenate([wide[:, SPECTRA + 2 * t + part : SPECTRA + 2 * t + part + 1] for t in range(slots)], 0)
        for part in range(2)
    ]
    tail = jnp.concatenate(tail + [jnp.zeros((HALF, 6), f32)], 1).T
    devices = arrived_ref.shape[0]
    row_sums = arrived_ref[...].reshape(devices, arrived_ref.shape[2])[:, arrived_ref.shape[2] - 4 * rows :]
    z = mm3((dft_high_ref[...], dft_low_ref[...]), pieces(row_sums[:, :rows]), TN)
    z_real, z_imag = z[:devices], -z[devices:]
    turns_of = [tuple(t[:, :rows] for t in twiddle(cos_ref, sin_ref, m)) for m in range(4)]
    zero = [
        jnp.concatenate([jnp.sum(z_real * c + z_imag * n, 1, keepdims=True) for c, n in turns_of], 0),
        jnp.concatenate([jnp.sum(z_imag * c - z_real * n, 1, keepdims=True) for c, n in turns_of], 0),
    ]
    lane = lane_index((1, HALF))
    frequency = 4 * (lane % (HALF // 4)) + lane // (HALF // 4) + 1
    last = lane == HALF - 1
    frequency_p = jnp.where(last, 0, frequency)
    across = row_index((K, 1)) - HALF
    across_m = jnp.where(across == -HALF, HALF, across)
    last_col = lane_index((K, HALF)) == HALF - 1
    first_row = row_index((K, HALF)) == 0
    for part in range(2):
        block = spectrum[part * K : (part + 1) * K]
        plus = jnp.where(last_col, zero[part], block)
        minus = jnp.where(first_row, tail[part : part + 1], block)
        for ref, value in ((plus_ref, plus), (minus_ref, minus)):
            high, low = pieces(value)
            ref[part * K : (part + 1) * K, :HALF] = high
            ref[part * K : (part + 1) * K, HALF:] = low

    def passes(s):
        s0 = shift_ref[s, 0]
        s1 = shift_ref[s, 1]
        a = across + s0
        b = frequency_p + s1
        plus = a * a <= radius_sq - b * b
        a = s0 - across_m
        b = s1 - frequency
        minus = a * a <= radius_sq - b * b
        return jnp.where(plus, 1.0, 0.0), jnp.where(minus, 1.0, 0.0)

    block = HALF // 4
    in_block = [lane_index((rows, HALF)) // block == i for i in range(4)]

    def place(choose):
        out = None
        for i in range(4):
            value, group = choose(i)
            value = pltpu.roll(value, (i - group) % 4 * block, 1) if i != group else value
            out = value if out is None else jnp.where(in_block[i], value, out)
        return out

    def lift(s, carry):
        parts = []
        for spec_ref, table_ref, passed in zip((plus_ref, minus_ref), (local_p_ref, local_m_ref), passes(s)):
            passed = passed.astype(bf16)
            passed = jnp.concatenate([passed, passed], 0)
            passed = jnp.concatenate([passed, passed], 1)
            out = mm(table_ref[...], spec_ref[...] * passed)
            out = (out[:half, :HALF] + out[half:, :HALF] + out[:half, HALF:]) * norming
            parts += [out[:rows], out[rows:]]
        at_rows = pl.ds(pl.multiple_of(s * rows, rows), rows)
        for e in range(4):
            groups = groups_of(e)
            high, low = pieces(place(lambda i: (parts[i], groups[i // 2])))
            lift_ref[at_rows, e * 2 * HALF : e * 2 * HALF + HALF] = high
            lift_ref[at_rows, e * 2 * HALF + HALF : (e + 1) * 2 * HALF] = low
        return carry

    lax.fori_loop(0, sources, lift, 0, unroll=16)
    field_tables = [
        (field_high_ref[e * HALF : (e + 1) * HALF], field_low_ref[e * HALF : (e + 1) * HALF]) for e in range(4)
    ]
    for e, (high, low) in enumerate(field_tables):
        lanes = slice(e * 2 * HALF, (e + 1) * 2 * HALF)
        packed = lift_ref[:, lanes]
        field_ref[:, lanes] = mm(packed, jnp.concatenate([high, high], 0)) + mm(packed[:, :HALF], low)

    def lane_blocks(at_rows):
        return [field_ref[at_rows, i * HALF : (i + 1) * HALF] for i in range(8)]

    def expose(s, total):
        at_rows = pl.ds(pl.multiple_of(s * rows, rows), rows)
        r0, i0, r1, i1, r2, i2, r3, i3 = lane_blocks(at_rows)
        real = [r0 + r2 + (r1 + r3), r0 - r2 - (i1 - i3), r0 + r2 - (r1 + r3), r0 - r2 + (i1 - i3)]
        imag = [i0 + i2 + (i1 + i3), i0 - i2 + (r1 - r3), i0 + i2 - (i1 + i3), i0 - i2 - (r1 - r3)]
        out = []
        for q in range(4):
            field_ref[at_rows, 2 * q * HALF : (2 * q + 1) * HALF] = real[q]
            field_ref[at_rows, (2 * q + 1) * HALF : (2 * q + 2) * HALF] = imag[q]
            out.append(total[q] + share_ref[s] * (real[q] * real[q] + imag[q] * imag[q]))
        return tuple(out)

    coarse = lax.fori_loop(0, sources, expose, (jnp.zeros((rows, HALF), f32),) * 4, unroll=16)
    spread = spread_high_ref[...], spread_low_ref[...]
    quarter = COARSE // 4
    spread = [tuple(t[at : at + n] for t in spread) for at, n in ((0, quarter), (quarter, quarter), (2 * quarter, 2 * quarter))]
    i0, i1, i2, i3 = coarse
    even, odd = i0 + i2, i1 + i3
    a, b = i0 - i2, i1 - i3
    e = mm3(pieces(even + odd), spread[0])
    f = mm3(pieces(even - odd), spread[1])
    rs = mm3(pieces(jnp.concatenate([jnp.concatenate([a, -b], 1), jnp.concatenate([b, a], 1)], 0)), spread[2])
    up, down = e + f, e - f
    r, t = rs[:rows], rs[rows:]
    fine = target_ref.shape[1] // 4
    slopes = []
    squares = jnp.zeros((rows, fine), f32)
    for q, intensity in enumerate((up + r, down + t, up - r, down - t)):
        resist = 1.0 / (1.0 + jnp.exp(-steepness * (intensity - threshold)))
        misfit = resist - target_ref[:, q * fine : (q + 1) * fine].astype(f32)
        slopes.append((2.0 * steepness) * misfit * resist * (1.0 - resist))
        squares = squares + misfit * misfit
    s0, s1, s2, s3 = slopes
    even, odd = s0 + s2, s1 + s3
    de = mm3(pieces(even + odd), spread[0], NT)
    df = mm3(pieces(even - odd), spread[1], NT)
    x = mm3(pieces(jnp.concatenate([s0 - s2, s1 - s3], 0)), spread[2], NT)
    da = x[:rows, :quarter] + x[rows:, quarter:]
    db = x[rows:, :quarter] - x[:rows, quarter:]
    up, down = de + df, de - df
    slope_c = [up + da, down + db, up - da, down - db]

    def lane_sum(a):
        a = jnp.sum(a, 0, keepdims=True)
        total = a[:, :128]
        for i in range(1, a.shape[1] // 128):
            total = total + a[:, i * 128 : (i + 1) * 128]
        return total

    sums_ref[...] = jnp.zeros(sums_ref.shape, f32)
    sums_ref[80:81, :] = lane_sum(squares)
    for ref in (pull_p_ref, pull_m_ref):
        ref[...] = jnp.zeros(ref.shape, f32)

    def push(s, carry):
        at_rows = pl.ds(pl.multiple_of(s * rows, rows), rows)
        blocks = lane_blocks(at_rows)
        bright = jnp.zeros((rows, HALF), f32)
        real, imag = [], []
        for q in range(4):
            re, im = blocks[2 * q], blocks[2 * q + 1]
            bright = bright + (re * re + im * im) * slope_c[q]
            factor = (2.0 * norming * share_ref[s]) * slope_c[q]
            real.append(factor * re)
            imag.append(factor * im)
        sums_ref[pl.ds(64 + s, 1), :] = jnp.sum(bright, 0, keepdims=True)
        er, ei, fr, fi = real[0] + real[2], imag[0] + imag[2], real[1] + real[3], imag[1] + imag[3]
        ar, ai, br, bi = real[0] - real[2], imag[0] - imag[2], real[1] - real[3], imag[1] - imag[3]
        turned = [er + fr, ei + fi, ar + bi, ai - br, er - fr, ei - fi, ar - bi, ai + br]
        for i, value in enumerate(turned):
            high, low = pieces(value)
            back_high_ref[at_rows, i * HALF : (i + 1) * HALF] = high
            back_low_ref[at_rows, i * HALF : (i + 1) * HALF] = low
        return carry

    lax.fori_loop(0, sources, push, 0, unroll=16)
    for e, (high, low) in enumerate(field_tables):
        lanes = slice(e * 2 * HALF, (e + 1) * 2 * HALF)
        both = mm(back_high_ref[:, lanes], jnp.concatenate([high, low], 0), NT)
        settled_ref[:, e * HALF : (e + 1) * HALF] = (
            both[:, :HALF] + both[:, HALF:] + mm(back_low_ref[:, lanes], high, NT)
        )

    def pull(s, carry):
        at_rows = pl.ds(pl.multiple_of(s * rows, rows), rows)
        settled = [settled_ref[at_rows, e * HALF : (e + 1) * HALF] for e in range(4)]
        arrays = [
            place(lambda i: (settled[(i + 1) % 4 if k < 2 else (3 - i) % 4], k)) for k in range(4)
        ]
        for pull_ref, table_ref, passed, at in zip(
            (pull_p_ref, pull_m_ref), (local_pt_ref, local_mt_ref), passes(s), (0, 2)
        ):
            high, low = pieces(jnp.concatenate(arrays[at : at + 2], 0))
            out = mm(table_ref[...], jnp.concatenate([high, low, high], 0))
            pull_ref[...] += out * jnp.concatenate([passed, passed], 0)
        return carry

    lax.fori_loop(0, sources, pull, 0, unroll=16)
    plus = pull_p_ref[...]
    minus = pull_m_ref[...]
    y_real = jnp.zeros((devices, rows), f32)
    y_imag = jnp.zeros((devices, rows), f32)
    for m, (c, n) in enumerate(turns_of):
        real = plus[m * devices : (m + 1) * devices, HALF - 1 :]
        imag = plus[K + m * devices : K + (m + 1) * devices, HALF - 1 :]
        y_real = y_real + (real * c - imag * n)
        y_imag = y_imag + (real * n + imag * c)
    turn = turn_high_ref[...], turn_low_ref[...]
    level = mm3(turn, pieces(jnp.concatenate([y_real, -y_imag], 0)))
    level = jnp.concatenate([level[f * owners : (f + 1) * owners] for f in range(FAR)], 1)
    sums = jnp.sum(sums_ref[...].T, 0, keepdims=True)
    lane = lane_index((owners, 128))
    tail = jnp.broadcast_to(sums, (owners, 128))
    edge = jnp.concatenate([minus[:1], minus[K : K + 1], jnp.zeros((6, HALF), f32)], 0).T
    for t in range(slots):
        for part in range(2):
            tail = jnp.where(lane == 2 * t + part, edge[t * owners : (t + 1) * owners, part : part + 1], tail)
    total = jnp.where(lane_index(plus.shape) == HALF - 1, 0.0, plus)
    total = total + jnp.where(row_index(plus.shape) % K == 0, 0.0, minus)
    total = total.T
    row = jnp.concatenate([total[t * owners : (t + 1) * owners] for t in range(slots)] + [tail, level], 1)
    low, high = row[:near], row[near:]
    out_mine_ref[...] = jnp.where(first_core, low, high).reshape(out_mine_ref.shape)
    out_theirs_ref[...] = jnp.where(first_core, high, low).reshape(out_theirs_ref.shape)


def owner_kernel(own_ref, in_ref, high_ref, low_ref, cos_ref, sin_ref, out_ref):
    total = jnp.sum(in_ref[...], 0)
    tail = total[:, SPECTRA : SPECTRA + 128]
    devices = out_ref.shape[0]
    rows = cos_ref.shape[1] // 4
    count = SPECTRA // K
    owners = devices // FAR
    columns = jnp.concatenate([total[:, q * K : (q + 1) * K] for q in range(count)], 0).T
    edge = jnp.where(row_index((8, count)) == 0, tail[:, :count], 0.0)
    columns = jnp.concatenate(pieces(jnp.concatenate([columns, edge], 0)), 1)
    lanes = count * rows
    have = row_index((2 * count, lanes)) % count
    want = lane_index((2 * count, lanes)) // rows
    straight = jnp.where(have == want, 1.0, 0.0)
    partner = jnp.where(want % 2 == 0, want + 1, want - 1)
    crossed = jnp.where(have == partner, jnp.where(want % 2 == 0, -1.0, 1.0), 0.0)
    straight = mm(columns, straight.astype(bf16))
    crossed = mm(columns, crossed.astype(bf16))
    z = jnp.zeros((devices, lanes), f32)
    for m in range(5):
        cos, sin = (jnp.concatenate([t] * (count // 4), 1) for t in twiddle(cos_ref, sin_ref, m))
        if m < 4:
            z = z + straight[m * devices : (m + 1) * devices] * cos + crossed[m * devices : (m + 1) * devices] * sin
        else:
            last = straight[K:] * cos[:8] + crossed[K:] * sin[:8]
            z = jnp.concatenate([z[:8] + last, z[8:]], 0)
    out = mm3((high_ref[...], low_ref[...]), pieces(jnp.concatenate([z, -swapped(z, rows)], 0)))
    device = row_index((devices, rows))
    level = jnp.zeros((devices, rows), f32)
    for f in range(FAR):
        at = SPECTRA + 128 + f * rows
        level = jnp.where(device // owners == f, total[:, at : at + rows], level)
    level = jnp.where(device % owners == own_ref[0], level, 0.0)
    extra = jnp.concatenate([level, jnp.broadcast_to(tail[:, rows:] * (1.0 / owners), (devices, 3 * rows))], 1)
    out_ref[...] = jnp.concatenate([out, extra], 1).reshape(out_ref.shape)


def grad_kernel(in_ref, share_ref, group_ref, high_ref, low_ref, out_ref, loss_ref, group_out_ref):
    rows, length = out_ref.shape
    quarter = length // 4
    devices, _, lanes = in_ref.shape
    owners = devices // FAR
    a = in_ref[...].reshape(devices, lanes)
    parts = [a[f * owners : (f + 1) * owners] for f in range(FAR)]
    a = (parts[0] + parts[1]) + (parts[2] + parts[3])
    none = jnp.zeros((owners, rows), f32)
    slots = HALF // owners
    by_cos, by_sin = [], []
    for t in range(slots):
        re, im = a[:, 2 * t * rows : (2 * t + 1) * rows], a[:, (2 * t + 1) * rows : (2 * t + 2) * rows]
        group = t * owners // (HALF // 4)
        by_cos += [jnp.concatenate(([none, none, re, -im], [none, re, none, none], [none, none, re, im], [re, none, none, none])[group], 1)]
        by_sin += [jnp.concatenate(([none, none, -im, -re], [none, -im, none, none], [none, none, -im, re], [-im, none, none, none])[group], 1)]
    stack = jnp.concatenate(by_cos + by_sin, 0).T
    both = mm3(pieces(stack), (high_ref[...], low_ref[...]))
    sums = jnp.sum(a[:, 2 * slots * rows :], 0, keepdims=True)
    const = jnp.broadcast_to(sums, (8, 128)).T[:rows, :1]
    e = both[:rows] + const
    f = both[rows : 2 * rows]
    g = both[2 * rows : 3 * rows]
    h = both[3 * rows :]
    up, down = e + f, e - f
    out_ref[:, :quarter] = up + g
    out_ref[:, quarter : 2 * quarter] = down + h
    out_ref[:, 2 * quarter : 3 * quarter] = up - g
    out_ref[:, 3 * quarter :] = down - h
    norming = 1.0 / (length * length)
    loss_ref[...] = sums[:, 80:81] * norming
    share = share_ref[...]
    against = jnp.sum(share * sums, 1, keepdims=True)
    pull = share * (sums - against) * norming
    group_out_ref[...] = jnp.sum((group_ref[...] * pull).T, 0, keepdims=True)


def tables(rows, length, near):
    devices = 2 * near * FAR
    owner = np.arange(2 * near)
    t = np.arange(HALF // len(owner))[:, None]
    place = t * len(owner) + (owner % 2) * near + owner // 2
    slots = (4 * (place % (HALF // 4)) + place // (HALF // 4) + 1).reshape(-1)
    cos, sin = turns(slots, np.arange(length // 4), length)
    row_table = np.concatenate([cos, sin], 0)
    cos, sin = turns(np.arange(devices), np.arange(devices), devices)
    dft = np.concatenate([cos, sin], 1)
    n = np.arange(near)
    in_order = np.concatenate([2 * near * f + 2 * n + c for f in range(FAR) for c in range(2)])
    turn = dft[in_order]
    across = np.concatenate([np.arange(devices), devices * np.arange(8) - HALF])
    cos, sin = turns(across, np.arange(rows), length)
    turning = np.tile(cos, (1, 4)).astype(np.float32), np.tile(sin, (1, 4)).astype(np.float32)
    samples = (length // COARSE) * np.arange(COARSE)
    group = HALF // 4
    lanes = np.concatenate([4 * np.arange(group) + g + 1 for g in range(4)])
    first = np.concatenate([lanes[:-1], [0]])
    cos_p, sin_p = turns(first, samples[: COARSE // 4], length)
    cos_m, sin_m = turns(lanes, samples[: COARSE // 4], length)
    field = []
    for e in range(4):
        p, m = (slice(g * group, (g + 1) * group) for g in groups_of(e))
        real = np.concatenate([cos_p[p], -sin_p[p], cos_m[m], -sin_m[m]], 0)
        imag = np.concatenate([sin_p[p], cos_p[p], -sin_m[m], -cos_m[m]], 0)
        field.append(np.concatenate([real, imag], 1))
    field = np.concatenate(field, 0)
    tones = np.arange(1, COARSE // 2 + 1)
    share = np.where(tones == COARSE // 2, 1.0, 2.0)
    pixels = np.arange(length)
    kernel = (1.0 + np.cos(2.0 * np.pi * (np.outer(pixels, tones) % length) / length) @ share) / COARSE
    spread = kernel.reshape(1, length).astype(np.float32)
    return host_pieces(row_table), host_pieces(dft), host_pieces(turn), turning, host_pieces(field), spread


def call(kernel, out_shape, scratch=(), n_scalar=0, n_in=0, mib=12, interpret=False):
    vmem = pl.BlockSpec(memory_space=pltpu.VMEM)
    smem = pl.BlockSpec(memory_space=pltpu.SMEM)
    multi = isinstance(out_shape, (tuple, list))
    return pl.pallas_call(
        kernel,
        out_shape=out_shape,
        in_specs=[smem] * n_scalar + [vmem] * n_in,
        out_specs=[vmem] * len(out_shape) if multi else vmem,
        scratch_shapes=list(scratch),
        compiler_params=pltpu.CompilerParams(vmem_limit_bytes=mib * 1024 * 1024),
        interpret=interpret,
    )


def image_scratch(sources, rows):
    vmem = pltpu.VMEM
    return [
        vmem((2 * K, 2 * HALF), bf16),
        vmem((2 * K, 2 * HALF), bf16),
        vmem((sources * rows, 8 * HALF), bf16),
        vmem((sources * rows, 2 * COARSE), f32),
        vmem((sources * rows, 2 * COARSE), bf16),
        vmem((sources * rows, 2 * COARSE), bf16),
        vmem((sources * rows, 4 * HALF), f32),
        vmem((2 * K, HALF), f32),
        vmem((2 * K, HALF), f32),
        vmem((128, 128), f32),
    ]


INTERPRET = False


def on_device(mask_field, target_print, source_points, source_groups, group_logits, pupil_radius):
    rows, length = mask_field.shape
    near = lax.axis_size(NEAR)
    pair = lax.axis_size(CORE)
    devices = FAR * near * pair
    sources = source_points.shape[0]
    row_table, dft, turn, turning, field, spread = tables(rows, length, near)
    device = lax.axis_index(SLAB)
    norming = 1.0 / (length * length)
    cutoff = pupil_radius[0]
    shifted = (source_points - GRID // 2) * cutoff // shift_scale
    shape = functools.partial(jax.ShapeDtypeStruct, dtype=f32)
    run = functools.partial(call, interpret=INTERPRET)

    def swap_all(parcels, axes):
        return lax.all_to_all(parcels, axes, split_axis=0, concat_axis=0, tiled=True)

    onehot = (source_groups[:, None] == jnp.arange(NG, dtype=jnp.int32)[None, :]).astype(f32)
    weights = jnp.exp(jnp.sum(onehot * group_logits[None, :], 1))
    total_weight = jnp.sum(weights)
    weight_share = weights / total_weight
    width = 2 * HALF // (near * pair) * rows + 4 * rows
    parcels = run(rows_kernel, shape((devices, 1, width)), n_in=3, mib=56)(mask_field, *row_table)
    arrived = swap_all(parcels, SLAB)
    across = jnp.arange(K, dtype=jnp.int32) - HALF
    here = device * rows + jnp.arange(rows, dtype=jnp.int32)
    angle = jnp.mod(here[:, None] * across[None, :], length).astype(f32) * (2.0 * np.pi / length)
    sizes = ((4 * rows, 2 * K),) * 2 + ((2 * K, 6 * rows),) * 2 + ((COARSE, length // 4),) * 2
    local_p, local_m, local_pt, local_mt, *spread, ready = run(
        local_kernel,
        tuple(jax.ShapeDtypeStruct(t, bf16) for t in sizes) + (shape((8, 128)),),
        n_in=3,
    )(jnp.cos(angle), jnp.sin(angle), spread)
    piece = run(columns_kernel, shape((near, 1, SPECTRA + 128)), n_in=7)(
        arrived, *dft, *turning, ready, weight_share.reshape(1, sources)
    )
    around = swap_all(piece, NEAR)
    theirs = lax.ppermute(around, CORE, [(i, (i + 1) % pair) for i in range(pair)])

    mine, theirs = run(
        image_kernel,
        (shape((near, 1, SPECTRA + 256)),) * 2,
        n_scalar=4,
        n_in=18,
        mib=28,
        scratch=image_scratch(sources, rows),
    )(
        shifted,
        weight_share,
        pupil_radius,
        lax.axis_index(CORE).reshape(1),
        around,
        theirs,
        arrived,
        *dft,
        *turn,
        *turning,
        local_p,
        local_m,
        local_pt,
        local_mt,
        *field,
        *spread,
        target_print,
    )
    mine = mine + lax.ppermute(theirs, CORE, [(i, (i + 1) % pair) for i in range(pair)])
    mine = swap_all(mine, NEAR)
    own = (lax.axis_index(NEAR) * pair + lax.axis_index(CORE)).reshape(1)
    parcels = run(owner_kernel, shape((devices, 1, width)), n_scalar=1, n_in=5)(own, mine, *dft, *turning)
    arrived = swap_all(parcels, SLAB)
    share_row = jnp.zeros((1, 128), f32).at[0, 64 : 64 + sources].set(weight_share)
    group_rows = jnp.zeros((NG, 128), f32).at[:, 64 : 64 + sources].set(onehot.T)
    mask_grad, loss_value, group_grad = run(
        grad_kernel, (shape((rows, length)), shape((1, 1)), shape((1, NG))), n_in=5
    )(arrived, share_row, group_rows, *row_table)
    return (loss_value.reshape(1), mask_grad, group_grad.reshape(NG))


def solution(mesh):
    cores = 2
    near = mesh.shape["slab"] // cores // FAR
    split = Mesh(mesh.devices.reshape(mesh.shape["clip"], FAR, near, cores), CLIP_SLAB)
    return jax.shard_map(
        on_device,
        mesh=split,
        in_specs=(
            P(CLIP_SLAB, None),
            P(CLIP_SLAB, None),
            P("clip", None),
            P("clip"),
            P("clip"),
            P("clip"),
        ),
        out_specs=(P("clip"), P(CLIP_SLAB, None), P("clip")),
        check_vma=False,
    )
```

```python
import functools

import numpy as np
import jax
import jax.numpy as jnp
from jax import lax
from jax.experimental import pallas as pl
from jax.experimental.pallas import tpu as pltpu
from jax.sharding import Mesh
from jax.sharding import PartitionSpec as P

K = 256
HALF = K // 2
GRID = 61
NG = 8
COARSE = 2 * K
FAR = 4
SPECTRA = K * K // 16
FAR_AXIS = "slab_0"
NEAR = "slab_1"
CORE = "slab_2"
SLAB = (FAR_AXIS, NEAR, CORE)
CLIP_SLAB = ("clip", *SLAB)

steepness = 8.0
threshold = 0.3
shift_scale = 45

f32 = jnp.float32
bf16 = jnp.bfloat16
NN = (((1,), (0,)), ((), ()))
NT = (((1,), (1,)), ((), ()))
TN = (((0,), (0,)), ((), ()))


def mm(a, b, dims=NN):
    return lax.dot_general(a, b, dims, preferred_element_type=f32)


def pieces(a):
    high = a.astype(bf16)
    return high, (a - high.astype(f32)).astype(bf16)


def mm3(a, b, dims=NN):
    return mm(a[0], b[0], dims) + mm(a[1], b[0], dims) + mm(a[0], b[1], dims)


def host_pieces(table):
    high = table.astype(np.float32).astype(jnp.bfloat16)
    low = (table - high.astype(np.float64)).astype(np.float32).astype(jnp.bfloat16)
    return np.asarray(high), np.asarray(low)


def turns(left, right, length):
    angle = 2.0 * np.pi * (np.outer(left, right) % length) / length
    return np.cos(angle), np.sin(angle)


def groups_of(e):
    return (e - 1) % 4, (3 - e) % 4


def lane_index(shape):
    return lax.broadcasted_iota(jnp.int32, shape, len(shape) - 1)


def row_index(shape):
    return lax.broadcasted_iota(jnp.int32, shape, 0)


def swapped(a, rows):
    lanes = a.shape[1]
    first = (lane_index(a.shape) // rows) % 2 == 0
    return jnp.where(first, pltpu.roll(a, lanes - rows, 1), -pltpu.roll(a, rows, 1))


def twiddle(cos_ref, sin_ref, m):
    owners = cos_ref.shape[0] - 8
    cos, sin = cos_ref[:owners], sin_ref[:owners]
    cos_m, sin_m = cos_ref[owners + m : owners + m + 1], sin_ref[owners + m : owners + m + 1]
    return cos * cos_m - sin * sin_m, sin * cos_m + cos * sin_m


def rows_kernel(core_ref, mask_ref, high_ref, low_ref, mine_ref, theirs_ref):
    rows, length = mask_ref.shape
    quarter = length // 4
    m0, m1, m2, m3 = (mask_ref[:, q * quarter : (q + 1) * quarter] for q in range(4))
    even, odd = m0 + m2, m1 + m3
    stack = jnp.concatenate([even + odd, even - odd, m0 - m2, m1 - m3], 0)
    stack = pieces(stack)
    both = mm3((high_ref[...], low_ref[...]), stack, NT)
    cos, sin = both[:HALF], both[HALF:]
    c0, c2, ca, cb = (cos[:, i * rows : (i + 1) * rows] for i in range(4))
    s0, s2, sa, sb = (sin[:, i * rows : (i + 1) * rows] for i in range(4))
    ones = jnp.ones((8, quarter), bf16)
    sums = (mm(ones, stack[0], NT) + mm(ones, stack[1], NT))[:1, :rows]
    group = HALF // 4
    g0, g1, g2, g3 = (slice(g * group, (g + 1) * group) for g in range(4))
    real = [ca[g0] - sb[g0], c2[g1], ca[g2] + sb[g2], c0[g3]]
    imag = [-sa[g0] - cb[g0], -s2[g1], cb[g2] - sa[g2], -s0[g3]]
    chips = mine_ref.shape[0] // FAR
    owners = 2 * chips
    slots = group // owners
    blocks = []
    for re, im in zip(real, imag):
        for t in range(slots):
            blocks += [re[t * owners : (t + 1) * owners], im[t * owners : (t + 1) * owners]]
    parcels = jnp.concatenate(blocks, 1)
    sums = jnp.broadcast_to(sums, (chips, rows))
    none = jnp.zeros((chips, rows), f32)
    first_core = core_ref[0] == 0
    low, high = parcels[:chips], parcels[chips:]
    empty = jnp.zeros(low.shape, f32)
    for out_ref, part in (
        (mine_ref, [jnp.where(first_core, low, high), empty, sums, none]),
        (theirs_ref, [empty, jnp.where(first_core, high, low), none, sums]),
    ):
        part = jnp.concatenate(part + [none, none], 1)
        out_ref[...] = jnp.concatenate([part] * FAR, 0).reshape(out_ref.shape)


def both_cores(first_core, own, other):
    return jnp.concatenate([jnp.where(first_core, own, other), jnp.where(first_core, other, own)], 0)


def local_kernel(
    cos_ref, sin_ref, kernel_ref, plus_ref, minus_ref, plus_t_ref, minus_t_ref, spread_high_ref, spread_low_ref, ready_ref
):
    cos = cos_ref[...]
    edge = lane_index(cos.shape) == 0
    for out_ref, out_t_ref, sin in (
        (plus_ref, plus_t_ref, sin_ref[...]),
        (minus_ref, minus_t_ref, jnp.where(edge, -sin_ref[...], sin_ref[...])),
    ):
        table = jnp.concatenate([jnp.concatenate([cos, -sin], 1), jnp.concatenate([sin, cos], 1)], 0)
        high, low = pieces(table)
        out_ref[...] = jnp.concatenate([high, low], 0)
        high, low = pieces(table.T)
        out_t_ref[...] = jnp.concatenate([high, high, low], 1)
    ready_ref[...] = cos[:8, :128]
    length = kernel_ref.shape[1]
    near, fine = COARSE // 4, length // 4
    at = pltpu.roll(
        jnp.broadcast_to(kernel_ref[...], (near, length)), 0, 1, stride=length // COARSE, stride_axis=0
    )
    h0, h1, h2, h3 = (at[:, p * fine : (p + 1) * fine] for p in range(4))
    even, odd = h0 + h2, h1 + h3
    for i, table in enumerate(((even + odd) / 4, (even - odd) / 4, (h0 - h2) / 2, (h1 - h3) / 2)):
        high, low = pieces(table)
        spread_high_ref[i * near : (i + 1) * near] = high
        spread_low_ref[i * near : (i + 1) * near] = low


def columns_kernel(core_ref, in_ref, dft_high_ref, dft_low_ref, cos_ref, sin_ref, ready_ref, share_ref, piece_ref):
    chips, _, lanes = in_ref.shape
    rows = cos_ref.shape[1] // 4
    lanes = (lanes - 4 * rows) // 2
    a = in_ref[...].reshape(chips, 2 * lanes + 4 * rows)
    a = both_cores(core_ref[0] == 0, a[:, :lanes], a[:, lanes : 2 * lanes])
    turn = dft_high_ref[...], dft_low_ref[...]
    devices = 2 * chips
    by_cos, by_sin = (tuple(t[:, i * devices : (i + 1) * devices] for t in turn) for i in range(2))
    z = mm3(by_cos, pieces(a), TN) + mm3(by_sin, pieces(swapped(a, rows)), TN)
    turned = swapped(z, rows)
    blocks = []
    for m in range(5):
        cos, sin = (jnp.concatenate([t] * (lanes // (4 * rows)), 1) for t in twiddle(cos_ref, sin_ref, m))
        blocks.append(z * cos + turned * sin)
    high, low = pieces(jnp.concatenate(blocks, 0))
    count = lanes // rows
    pick = (row_index((count, lanes)) == lane_index((count, lanes)) // rows).astype(f32).astype(bf16)
    sums = mm(pick, high, NT) + mm(pick, low, NT)
    copies = piece_ref.shape[0]
    lane = lane_index((1, 128))
    tail = jnp.zeros((1, 128), f32)
    for q in range(count):
        tail = jnp.where(lane == q, sums[q : q + 1, K : K + 1], tail)
    row = jnp.concatenate([sums[q : q + 1, :K] for q in range(count)] + [tail], 1)
    piece_ref[...] = jnp.broadcast_to(row.reshape(1, 1, row.shape[1]), (copies, 1, row.shape[1]))


def image_kernel(
    shift_ref,
    share_ref,
    radius_ref,
    core_ref,
    mine_ref,
    theirs_ref,
    arrived_ref,
    dft_high_ref,
    dft_low_ref,
    turn_high_ref,
    turn_low_ref,
    cos_ref,
    sin_ref,
    local_p_ref,
    local_m_ref,
    local_pt_ref,
    local_mt_ref,
    field_high_ref,
    field_low_ref,
    spread_high_ref,
    spread_low_ref,
    target_ref,
    out_mine_ref,
    out_theirs_ref,
    plus_ref,
    minus_ref,
    lift_ref,
    field_ref,
    back_high_ref,
    back_low_ref,
    settled_ref,
    pull_p_ref,
    pull_m_ref,
    sums_ref,
):
    sources = shift_ref.shape[0]
    rows = target_ref.shape[0]
    half = 2 * rows
    norming = 1.0 / (target_ref.shape[1] * target_ref.shape[1])
    radius_sq = radius_ref[0] * radius_ref[0]
    first_core = core_ref[0] == 0
    near = mine_ref.shape[0]
    mine = mine_ref[...].reshape(near, SPECTRA + 128)
    theirs = theirs_ref[...].reshape(near, SPECTRA + 128)
    wide = jnp.concatenate([jnp.where(first_core, mine, theirs), jnp.where(first_core, theirs, mine)], 0)
    owners = 2 * near
    slots = HALF // owners
    body = jnp.concatenate([wide[:, t * 2 * K : (t + 1) * 2 * K] for t in range(slots)], 0)
    spectrum = body.T
    tail = [
        jnp.concatenate([wide[:, SPECTRA + 2 * t + part : SPECTRA + 2 * t + part + 1] for t in range(slots)], 0)
        for part in range(2)
    ]
    tail = jnp.concatenate(tail + [jnp.zeros((HALF, 6), f32)], 1).T
    chips, _, lanes = arrived_ref.shape
    devices = 2 * chips
    row_sums = arrived_ref[...].reshape(chips, lanes)[:, lanes - 4 * rows :]
    row_sums = both_cores(first_core, row_sums[:, :rows], row_sums[:, rows : 2 * rows])
    z = mm3((dft_high_ref[...], dft_low_ref[...]), pieces(row_sums), TN)
    z_real, z_imag = z[:devices], -z[devices:]
    turns_of = [tuple(t[:, :rows] for t in twiddle(cos_ref, sin_ref, m)) for m in range(4)]
    zero = [
        jnp.concatenate([jnp.sum(z_real * c + z_imag * n, 1, keepdims=True) for c, n in turns_of], 0),
        jnp.concatenate([jnp.sum(z_imag * c - z_real * n, 1, keepdims=True) for c, n in turns_of], 0),
    ]
    lane = lane_index((1, HALF))
    frequency = 4 * (lane % (HALF // 4)) + lane // (HALF // 4) + 1
    last = lane == HALF - 1
    frequency_p = jnp.where(last, 0, frequency)
    across = row_index((K, 1)) - HALF
    across_m = jnp.where(across == -HALF, HALF, across)
    last_col = lane_index((K, HALF)) == HALF - 1
    first_row = row_index((K, HALF)) == 0
    for part in range(2):
        block = spectrum[part * K : (part + 1) * K]
        plus = jnp.where(last_col, zero[part], block)
        minus = jnp.where(first_row, tail[part : part + 1], block)
        for ref, value in ((plus_ref, plus), (minus_ref, minus)):
            high, low = pieces(value)
            ref[part * K : (part + 1) * K, :HALF] = high
            ref[part * K : (part + 1) * K, HALF:] = low

    def passes(s):
        s0 = shift_ref[s, 0]
        s1 = shift_ref[s, 1]
        a = across + s0
        b = frequency_p + s1
        plus = a * a <= radius_sq - b * b
        a = s0 - across_m
        b = s1 - frequency
        minus = a * a <= radius_sq - b * b
        return jnp.where(plus, 1.0, 0.0), jnp.where(minus, 1.0, 0.0)

    block = HALF // 4
    in_block = [lane_index((rows, HALF)) // block == i for i in range(4)]

    def place(choose):
        out = None
        for i in range(4):
            value, group = choose(i)
            value = pltpu.roll(value, (i - group) % 4 * block, 1) if i != group else value
            out = value if out is None else jnp.where(in_block[i], value, out)
        return out

    def lift(s, carry):
        parts = []
        for spec_ref, table_ref, passed in zip((plus_ref, minus_ref), (local_p_ref, local_m_ref), passes(s)):
            passed = passed.astype(bf16)
            passed = jnp.concatenate([passed, passed], 0)
            passed = jnp.concatenate([passed, passed], 1)
            out = mm(table_ref[...], spec_ref[...] * passed)
            out = (out[:half, :HALF] + out[half:, :HALF] + out[:half, HALF:]) * norming
            parts += [out[:rows], out[rows:]]
        at_rows = pl.ds(pl.multiple_of(s * rows, rows), rows)
        for e in range(4):
            groups = groups_of(e)
            high, low = pieces(place(lambda i: (parts[i], groups[i // 2])))
            lift_ref[at_rows, e * 2 * HALF : e * 2 * HALF + HALF] = high
            lift_ref[at_rows, e * 2 * HALF + HALF : (e + 1) * 2 * HALF] = low
        return carry

    lax.fori_loop(0, sources, lift, 0, unroll=16)
    field_tables = [
        (field_high_ref[e * HALF : (e + 1) * HALF], field_low_ref[e * HALF : (e + 1) * HALF]) for e in range(4)
    ]
    for e, (high, low) in enumerate(field_tables):
        lanes = slice(e * 2 * HALF, (e + 1) * 2 * HALF)
        packed = lift_ref[:, lanes]
        field_ref[:, lanes] = mm(packed, jnp.concatenate([high, high], 0)) + mm(packed[:, :HALF], low)

    def lane_blocks(at_rows):
        return [field_ref[at_rows, i * HALF : (i + 1) * HALF] for i in range(8)]

    def expose(s, total):
        at_rows = pl.ds(pl.multiple_of(s * rows, rows), rows)
        r0, i0, r1, i1, r2, i2, r3, i3 = lane_blocks(at_rows)
        real = [r0 + r2 + (r1 + r3), r0 - r2 - (i1 - i3), r0 + r2 - (r1 + r3), r0 - r2 + (i1 - i3)]
        imag = [i0 + i2 + (i1 + i3), i0 - i2 + (r1 - r3), i0 + i2 - (i1 + i3), i0 - i2 - (r1 - r3)]
        out = []
        for q in range(4):
            field_ref[at_rows, 2 * q * HALF : (2 * q + 1) * HALF] = real[q]
            field_ref[at_rows, (2 * q + 1) * HALF : (2 * q + 2) * HALF] = imag[q]
            out.append(total[q] + share_ref[s] * (real[q] * real[q] + imag[q] * imag[q]))
        return tuple(out)

    coarse = lax.fori_loop(0, sources, expose, (jnp.zeros((rows, HALF), f32),) * 4, unroll=16)
    spread = spread_high_ref[...], spread_low_ref[...]
    quarter = COARSE // 4
    spread = [tuple(t[at : at + n] for t in spread) for at, n in ((0, quarter), (quarter, quarter), (2 * quarter, 2 * quarter))]
    i0, i1, i2, i3 = coarse
    even, odd = i0 + i2, i1 + i3
    a, b = i0 - i2, i1 - i3
    e = mm3(pieces(even + odd), spread[0])
    f = mm3(pieces(even - odd), spread[1])
    rs = mm3(pieces(jnp.concatenate([jnp.concatenate([a, -b], 1), jnp.concatenate([b, a], 1)], 0)), spread[2])
    up, down = e + f, e - f
    r, t = rs[:rows], rs[rows:]
    fine = target_ref.shape[1] // 4
    slopes = []
    squares = jnp.zeros((rows, fine), f32)
    for q, intensity in enumerate((up + r, down + t, up - r, down - t)):
        resist = 1.0 / (1.0 + jnp.exp(-steepness * (intensity - threshold)))
        misfit = resist - target_ref[:, q * fine : (q + 1) * fine].astype(f32)
        slopes.append((2.0 * steepness) * misfit * resist * (1.0 - resist))
        squares = squares + misfit * misfit
    s0, s1, s2, s3 = slopes
    even, odd = s0 + s2, s1 + s3
    de = mm3(pieces(even + odd), spread[0], NT)
    df = mm3(pieces(even - odd), spread[1], NT)
    x = mm3(pieces(jnp.concatenate([s0 - s2, s1 - s3], 0)), spread[2], NT)
    da = x[:rows, :quarter] + x[rows:, quarter:]
    db = x[rows:, :quarter] - x[:rows, quarter:]
    up, down = de + df, de - df
    slope_c = [up + da, down + db, up - da, down - db]

    def lane_sum(a):
        a = jnp.sum(a, 0, keepdims=True)
        total = a[:, :128]
        for i in range(1, a.shape[1] // 128):
            total = total + a[:, i * 128 : (i + 1) * 128]
        return total

    sums_ref[...] = jnp.zeros(sums_ref.shape, f32)
    sums_ref[80:81, :] = lane_sum(squares)
    for ref in (pull_p_ref, pull_m_ref):
        ref[...] = jnp.zeros(ref.shape, f32)

    def push(s, carry):
        at_rows = pl.ds(pl.multiple_of(s * rows, rows), rows)
        blocks = lane_blocks(at_rows)
        bright = jnp.zeros((rows, HALF), f32)
        real, imag = [], []
        for q in range(4):
            re, im = blocks[2 * q], blocks[2 * q + 1]
            bright = bright + (re * re + im * im) * slope_c[q]
            factor = (2.0 * norming * share_ref[s]) * slope_c[q]
            real.append(factor * re)
            imag.append(factor * im)
        sums_ref[pl.ds(64 + s, 1), :] = jnp.sum(bright, 0, keepdims=True)
        er, ei, fr, fi = real[0] + real[2], imag[0] + imag[2], real[1] + real[3], imag[1] + imag[3]
        ar, ai, br, bi = real[0] - real[2], imag[0] - imag[2], real[1] - real[3], imag[1] - imag[3]
        turned = [er + fr, ei + fi, ar + bi, ai - br, er - fr, ei - fi, ar - bi, ai + br]
        for i, value in enumerate(turned):
            high, low = pieces(value)
            back_high_ref[at_rows, i * HALF : (i + 1) * HALF] = high
            back_low_ref[at_rows, i * HALF : (i + 1) * HALF] = low
        return carry

    lax.fori_loop(0, sources, push, 0, unroll=16)
    for e, (high, low) in enumerate(field_tables):
        lanes = slice(e * 2 * HALF, (e + 1) * 2 * HALF)
        both = mm(back_high_ref[:, lanes], jnp.concatenate([high, low], 0), NT)
        settled_ref[:, e * HALF : (e + 1) * HALF] = (
            both[:, :HALF] + both[:, HALF:] + mm(back_low_ref[:, lanes], high, NT)
        )

    def pull(s, carry):
        at_rows = pl.ds(pl.multiple_of(s * rows, rows), rows)
        settled = [settled_ref[at_rows, e * HALF : (e + 1) * HALF] for e in range(4)]
        arrays = [
            place(lambda i: (settled[(i + 1) % 4 if k < 2 else (3 - i) % 4], k)) for k in range(4)
        ]
        for pull_ref, table_ref, passed, at in zip(
            (pull_p_ref, pull_m_ref), (local_pt_ref, local_mt_ref), passes(s), (0, 2)
        ):
            high, low = pieces(jnp.concatenate(arrays[at : at + 2], 0))
            out = mm(table_ref[...], jnp.concatenate([high, low, high], 0))
            pull_ref[...] += out * jnp.concatenate([passed, passed], 0)
        return carry

    lax.fori_loop(0, sources, pull, 0, unroll=16)
    plus = pull_p_ref[...]
    minus = pull_m_ref[...]
    y_real = jnp.zeros((devices, rows), f32)
    y_imag = jnp.zeros((devices, rows), f32)
    for m, (c, n) in enumerate(turns_of):
        real = plus[m * devices : (m + 1) * devices, HALF - 1 :]
        imag = plus[K + m * devices : K + (m + 1) * devices, HALF - 1 :]
        y_real = y_real + (real * c - imag * n)
        y_imag = y_imag + (real * n + imag * c)
    turn = turn_high_ref[...], turn_low_ref[...]
    level = mm3(turn, pieces(jnp.concatenate([y_real, -y_imag], 0)))
    level = jnp.concatenate([level[f * owners : (f + 1) * owners] for f in range(FAR)], 1)
    sums = jnp.sum(sums_ref[...].T, 0, keepdims=True)
    lane = lane_index((owners, 128))
    tail = jnp.broadcast_to(sums, (owners, 128))
    edge = jnp.concatenate([minus[:1], minus[K : K + 1], jnp.zeros((6, HALF), f32)], 0).T
    for t in range(slots):
        for part in range(2):
            tail = jnp.where(lane == 2 * t + part, edge[t * owners : (t + 1) * owners, part : part + 1], tail)
    total = jnp.where(lane_index(plus.shape) == HALF - 1, 0.0, plus)
    total = total + jnp.where(row_index(plus.shape) % K == 0, 0.0, minus)
    total = total.T
    row = jnp.concatenate([total[t * owners : (t + 1) * owners] for t in range(slots)] + [tail, level], 1)
    low, high = row[:near], row[near:]
    out_mine_ref[...] = jnp.where(first_core, low, high).reshape(out_mine_ref.shape)
    out_theirs_ref[...] = jnp.where(first_core, high, low).reshape(out_theirs_ref.shape)


def owner_kernel(core_ref, near_ref, in_ref, high_ref, low_ref, cos_ref, sin_ref, mine_ref, theirs_ref):
    total = jnp.sum(in_ref[...], 0)
    tail = total[:, SPECTRA : SPECTRA + 128]
    chips = mine_ref.shape[0]
    devices = 2 * chips
    rows = cos_ref.shape[1] // 4
    count = SPECTRA // K
    owners = devices // FAR
    columns = jnp.concatenate([total[:, q * K : (q + 1) * K] for q in range(count)], 0).T
    edge = jnp.where(row_index((8, count)) == 0, tail[:, :count], 0.0)
    columns = jnp.concatenate(pieces(jnp.concatenate([columns, edge], 0)), 1)
    lanes = count * rows
    have = row_index((2 * count, lanes)) % count
    want = lane_index((2 * count, lanes)) // rows
    straight = jnp.where(have == want, 1.0, 0.0)
    partner = jnp.where(want % 2 == 0, want + 1, want - 1)
    crossed = jnp.where(have == partner, jnp.where(want % 2 == 0, -1.0, 1.0), 0.0)
    straight = mm(columns, straight.astype(bf16))
    crossed = mm(columns, crossed.astype(bf16))
    z = jnp.zeros((devices, lanes), f32)
    for m in range(5):
        cos, sin = (jnp.concatenate([t] * (count // 4), 1) for t in twiddle(cos_ref, sin_ref, m))
        if m < 4:
            z = z + straight[m * devices : (m + 1) * devices] * cos + crossed[m * devices : (m + 1) * devices] * sin
        else:
            last = straight[K:] * cos[:8] + crossed[K:] * sin[:8]
            z = jnp.concatenate([z[:8] + last, z[8:]], 0)
    out = mm3((high_ref[...], low_ref[...]), pieces(jnp.concatenate([z, -swapped(z, rows)], 0)))
    near = chips // FAR
    chip = row_index((chips, rows))
    level = jnp.zeros((chips, rows), f32)
    for f in range(FAR):
        at = SPECTRA + 128 + f * rows
        level = jnp.where(chip // near == f, total[:, at : at + rows], level)
    level = jnp.where(chip % near == near_ref[0], level, 0.0)
    scalars = jnp.broadcast_to(tail[:, rows:] * (1.0 / owners), (chips, 3 * rows))
    first_core = core_ref[0] == 0
    low, high = out[:chips], out[chips:]
    empty = jnp.zeros(low.shape, f32)
    mine = jnp.concatenate([jnp.where(first_core, low, high), empty, level, scalars], 1)
    theirs = jnp.concatenate([empty, jnp.where(first_core, high, low), jnp.zeros((chips, rows), f32), scalars], 1)
    mine_ref[...] = mine.reshape(mine_ref.shape)
    theirs_ref[...] = theirs.reshape(theirs_ref.shape)


def grad_kernel(core_ref, in_ref, share_ref, group_ref, high_ref, low_ref, out_ref, loss_ref, group_out_ref):
    rows, length = out_ref.shape
    quarter = length // 4
    chips, _, lanes = in_ref.shape
    near = chips // FAR
    owners = 2 * near
    a = in_ref[...].reshape(chips, lanes)
    parts = [a[f * near : (f + 1) * near] for f in range(FAR)]
    a = (parts[0] + parts[1]) + (parts[2] + parts[3])
    extra = a[:, lanes - 4 * rows :]
    lanes = (lanes - 4 * rows) // 2
    a = both_cores(core_ref[0] == 0, a[:, :lanes], a[:, lanes : 2 * lanes])
    none = jnp.zeros((owners, rows), f32)
    slots = HALF // owners
    by_cos, by_sin = [], []
    for t in range(slots):
        re, im = a[:, 2 * t * rows : (2 * t + 1) * rows], a[:, (2 * t + 1) * rows : (2 * t + 2) * rows]
        group = t * owners // (HALF // 4)
        by_cos += [jnp.concatenate(([none, none, re, -im], [none, re, none, none], [none, none, re, im], [re, none, none, none])[group], 1)]
        by_sin += [jnp.concatenate(([none, none, -im, -re], [none, -im, none, none], [none, none, -im, re], [-im, none, none, none])[group], 1)]
    stack = jnp.concatenate(by_cos + by_sin, 0).T
    both = mm3(pieces(stack), (high_ref[...], low_ref[...]))
    sums = jnp.sum(extra, 0, keepdims=True)
    const = jnp.broadcast_to(sums, (8, 128)).T[:rows, :1]
    e = both[:rows] + const
    f = both[rows : 2 * rows]
    g = both[2 * rows : 3 * rows]
    h = both[3 * rows :]
    up, down = e + f, e - f
    out_ref[:, :quarter] = up + g
    out_ref[:, quarter : 2 * quarter] = down + h
    out_ref[:, 2 * quarter : 3 * quarter] = up - g
    out_ref[:, 3 * quarter :] = down - h
    norming = 1.0 / (length * length)
    loss_ref[...] = sums[:, 80:81] * norming
    share = share_ref[...]
    against = jnp.sum(share * sums, 1, keepdims=True)
    pull = share * (sums - against) * norming
    group_out_ref[...] = jnp.sum((group_ref[...] * pull).T, 0, keepdims=True)


def tables(rows, length, near):
    devices = 2 * near * FAR
    place = np.arange(HALF)
    slots = 4 * (place % (HALF // 4)) + place // (HALF // 4) + 1
    cos, sin = turns(slots, np.arange(length // 4), length)
    row_table = np.concatenate([cos, sin], 0)
    cos, sin = turns(np.arange(devices), np.arange(devices), devices)
    dft = np.concatenate([cos, sin], 1)
    n = np.arange(near)
    in_order = np.concatenate([2 * near * f + 2 * n + c for f in range(FAR) for c in range(2)])
    turn = dft[in_order]
    dft = dft[np.concatenate([np.arange(0, devices, 2), np.arange(1, devices, 2)])]
    across = np.concatenate([np.arange(devices), devices * np.arange(8) - HALF])
    cos, sin = turns(across, np.arange(rows), length)
    turning = np.tile(cos, (1, 4)).astype(np.float32), np.tile(sin, (1, 4)).astype(np.float32)
    samples = (length // COARSE) * np.arange(COARSE)
    group = HALF // 4
    lanes = np.concatenate([4 * np.arange(group) + g + 1 for g in range(4)])
    first = np.concatenate([lanes[:-1], [0]])
    cos_p, sin_p = turns(first, samples[: COARSE // 4], length)
    cos_m, sin_m = turns(lanes, samples[: COARSE // 4], length)
    field = []
    for e in range(4):
        p, m = (slice(g * group, (g + 1) * group) for g in groups_of(e))
        real = np.concatenate([cos_p[p], -sin_p[p], cos_m[m], -sin_m[m]], 0)
        imag = np.concatenate([sin_p[p], cos_p[p], -sin_m[m], -cos_m[m]], 0)
        field.append(np.concatenate([real, imag], 1))
    field = np.concatenate(field, 0)
    tones = np.arange(1, COARSE // 2 + 1)
    share = np.where(tones == COARSE // 2, 1.0, 2.0)
    pixels = np.arange(length)
    kernel = (1.0 + np.cos(2.0 * np.pi * (np.outer(pixels, tones) % length) / length) @ share) / COARSE
    spread = kernel.reshape(1, length).astype(np.float32)
    return host_pieces(row_table), host_pieces(dft), host_pieces(turn), turning, host_pieces(field), spread


def call(kernel, out_shape, scratch=(), n_scalar=0, n_in=0, mib=12, interpret=False):
    vmem = pl.BlockSpec(memory_space=pltpu.VMEM)
    smem = pl.BlockSpec(memory_space=pltpu.SMEM)
    multi = isinstance(out_shape, (tuple, list))
    return pl.pallas_call(
        kernel,
        out_shape=out_shape,
        in_specs=[smem] * n_scalar + [vmem] * n_in,
        out_specs=[vmem] * len(out_shape) if multi else vmem,
        scratch_shapes=list(scratch),
        compiler_params=pltpu.CompilerParams(vmem_limit_bytes=mib * 1024 * 1024),
        interpret=interpret,
    )


def image_scratch(sources, rows):
    vmem = pltpu.VMEM
    return [
        vmem((2 * K, 2 * HALF), bf16),
        vmem((2 * K, 2 * HALF), bf16),
        vmem((sources * rows, 8 * HALF), bf16),
        vmem((sources * rows, 2 * COARSE), f32),
        vmem((sources * rows, 2 * COARSE), bf16),
        vmem((sources * rows, 2 * COARSE), bf16),
        vmem((sources * rows, 4 * HALF), f32),
        vmem((2 * K, HALF), f32),
        vmem((2 * K, HALF), f32),
        vmem((128, 128), f32),
    ]


INTERPRET = False


def on_device(mask_field, target_print, source_points, source_groups, group_logits, pupil_radius):
    rows, length = mask_field.shape
    near = lax.axis_size(NEAR)
    pair = lax.axis_size(CORE)
    devices = FAR * near * pair
    sources = source_points.shape[0]
    row_table, dft, turn, turning, field, spread = tables(rows, length, near)
    device = lax.axis_index(SLAB)
    norming = 1.0 / (length * length)
    cutoff = pupil_radius[0]
    shifted = (source_points - GRID // 2) * cutoff // shift_scale
    shape = functools.partial(jax.ShapeDtypeStruct, dtype=f32)
    run = functools.partial(call, interpret=INTERPRET)

    def swap_all(parcels, axes):
        return lax.all_to_all(parcels, axes, split_axis=0, concat_axis=0, tiled=True)

    onehot = (source_groups[:, None] == jnp.arange(NG, dtype=jnp.int32)[None, :]).astype(f32)
    weights = jnp.exp(jnp.sum(onehot * group_logits[None, :], 1))
    total_weight = jnp.sum(weights)
    weight_share = weights / total_weight
    width = 4 * HALF // (near * pair) * rows + 4 * rows
    core = lax.axis_index(CORE).reshape(1)

    def swap_rows(mine, theirs):
        theirs = lax.ppermute(theirs, CORE, [(i, (i + 1) % pair) for i in range(pair)])
        return swap_all(mine + theirs, (FAR_AXIS, NEAR))

    chips = FAR * near
    halves = (shape((chips, 1, width)),) * 2
    arrived = swap_rows(*run(rows_kernel, halves, n_scalar=1, n_in=3, mib=56)(core, mask_field, *row_table))
    across = jnp.arange(K, dtype=jnp.int32) - HALF
    here = device * rows + jnp.arange(rows, dtype=jnp.int32)
    angle = jnp.mod(here[:, None] * across[None, :], length).astype(f32) * (2.0 * np.pi / length)
    sizes = ((4 * rows, 2 * K),) * 2 + ((2 * K, 6 * rows),) * 2 + ((COARSE, length // 4),) * 2
    local_p, local_m, local_pt, local_mt, *spread, ready = run(
        local_kernel,
        tuple(jax.ShapeDtypeStruct(t, bf16) for t in sizes) + (shape((8, 128)),),
        n_in=3,
    )(jnp.cos(angle), jnp.sin(angle), spread)
    piece = run(columns_kernel, shape((near, 1, SPECTRA + 128)), n_scalar=1, n_in=7)(
        core, arrived, *dft, *turning, ready, weight_share.reshape(1, sources)
    )
    around = swap_all(piece, NEAR)
    theirs = lax.ppermute(around, CORE, [(i, (i + 1) % pair) for i in range(pair)])

    mine, theirs = run(
        image_kernel,
        (shape((near, 1, SPECTRA + 256)),) * 2,
        n_scalar=4,
        n_in=18,
        mib=28,
        scratch=image_scratch(sources, rows),
    )(
        shifted,
        weight_share,
        pupil_radius,
        core,
        around,
        theirs,
        arrived,
        *dft,
        *turn,
        *turning,
        local_p,
        local_m,
        local_pt,
        local_mt,
        *field,
        *spread,
        target_print,
    )
    mine = mine + lax.ppermute(theirs, CORE, [(i, (i + 1) % pair) for i in range(pair)])
    mine = swap_all(mine, NEAR)
    arrived = swap_rows(
        *run(owner_kernel, halves, n_scalar=2, n_in=5)(core, lax.axis_index(NEAR).reshape(1), mine, *dft, *turning)
    )
    share_row = jnp.zeros((1, 128), f32).at[0, 64 : 64 + sources].set(weight_share)
    group_rows = jnp.zeros((NG, 128), f32).at[:, 64 : 64 + sources].set(onehot.T)
    mask_grad, loss_value, group_grad = run(
        grad_kernel, (shape((rows, length)), shape((1, 1)), shape((1, NG))), n_scalar=1, n_in=5
    )(core, arrived, share_row, group_rows, *row_table)
    return (loss_value.reshape(1), mask_grad, group_grad.reshape(NG))


def solution(mesh):
    cores = 2
    near = mesh.shape["slab"] // cores // FAR
    split = Mesh(mesh.devices.reshape(mesh.shape["clip"], FAR, near, cores), CLIP_SLAB)
    return jax.shard_map(
        on_device,
        mesh=split,
        in_specs=(
            P(CLIP_SLAB, None),
            P(CLIP_SLAB, None),
            P("clip", None),
            P("clip"),
            P("clip"),
            P("clip"),
        ),
        out_specs=(P("clip"), P(CLIP_SLAB, None), P("clip")),
        check_vma=False,
    )
```
